32 devices in a mesh: grp: 2 (over y), lon: 16 (over z, x, core), lat: 1.
Axes of the slice: x: 2, y: 2, z: 4, core: 2. Of those that a mesh axis runs over, the one named last changes fastest.
Arguments:
- surface_field: bfloat16 [256, 128, 256], P(('grp', 'lat'), 'lon'), parts along dimension 0, may hold values from -6 to 6
- conv_a: bfloat16 [3, 3, 256, 512], replicated, may hold values from -0.125 to 0.125
- conv_b: bfloat16 [3, 3, 512, 512], replicated, may hold values from -0.09375 to 0.09375
- norm_gain: float32 [512], replicated, may hold values from 0.1 to 1.9
- qkv_weight: bfloat16 [512, 3072], replicated, may hold values from -3 to 3, as said below
- out_weight: bfloat16 [1024, 512], replicated, may hold values from -0.1875 to 0.1875
Outputs:
- mixed_out: bfloat16 [64, 32, 512], P(('grp', 'lat'), 'lon'), parts along dimension 0
The draws below stay inside these ranges and needn't reach their ends.
There are 2 independent parts, one for each index of `grp`. The reference program is written for one: setup_inputs(seed, part) draws one part's arguments, and reference() takes and returns one part's arrays. A program takes and returns all parts, laid end to end along the dimension named above; an argument that names none is the same for every part. Nothing has to cross between parts.
Inputs may be any that keep to these rules, and one draw needn't show every extreme that they name: `qkv_weight`: columns hold queries, keys and values in that order, each 16 heads of 64 entries.
All inputs are finite; a program needn't handle non-finite values.
Results may differ from the reference program's by a relative error of at most 0.012.
The reference program's roundings to bfloat16 on the way (of `pooled_first`, `normed`, `projected`, `weights` and `attended`) count: a program that leaves them out, or rounds other values in their place, can miss the bound.
Values may be sent and summed in bfloat16 or wider, within the bound.
A program may use at most 128 MiB of HBM per device.

```python
import math
import jax
import jax.numpy as jnp
from jax import lax

CA = 256
CB = 512
HEADS = 16
HEAD_DIM = 64
WIDTH = 1024
HA = 128
WA = 128


def draw_qkv_weight(key, part):
    key_query = jax.random.fold_in(key, 0)
    fan_scale = CB ** (-0.5)
    drawn = jnp.clip(jax.random.normal(key_query, (CB, 3 * HEADS * HEAD_DIM), jnp.float32) * 1.7, -6.0, 6.0) * fan_scale
    return drawn.astype(jnp.bfloat16)


def levels(rng, dims, cuts, low, top_value):
    def one(position, shards_of):
        draws = jax.random.uniform(jax.random.fold_in(jax.random.fold_in(rng, 6), position), (shards_of,), jnp.float32, low / len(cuts), top_value / len(cuts))
        return jnp.repeat(jnp.exp(draws), dims[position] // shards_of).reshape((-1,) + (1,) * (len(dims) - position - 1))

    loudness = one(*cuts[0])
    for cut in cuts[1:]:
        loudness = loudness * one(*cut)
    return loudness


def bell_draw(key, dims, scale, most, pieces=(), held_as=jnp.bfloat16):
    factor_of = levels(key, dims, pieces, -0.22, 0.18) if pieces else 1.0
    values = jax.random.normal(key, dims, jnp.float32) * scale * factor_of
    return jnp.minimum(jnp.maximum(values, -most), most).astype(held_as)


def setup_inputs(seed: int = 0, part: int = 0) -> dict:
    keys = jax.random.split(jax.random.key(seed), 7)
    part_keys = jax.random.split(jax.random.fold_in(keys[6], part), 7)
    surface_field = bell_draw(part_keys[0], (HA, WA, CA), 1.0, 6.0, ((1, 16),))
    conv_a = bell_draw(keys[1], (3, 3, CA, CB), (9 * CA) ** -0.5, 0.125)
    conv_b = bell_draw(keys[2], (3, 3, CB, CB), (9 * CB) ** -0.5, 0.09375)
    norm_gain = jnp.clip(1.0 + 0.18 * jax.random.normal(keys[3], (CB,), jnp.float32), 0.1, 1.9)
    qkv_weight = draw_qkv_weight(jax.random.fold_in(keys[6], 71), part)
    out_weight = bell_draw(keys[5], (WIDTH, CB), WIDTH ** -0.5, 0.1875)
    return dict(surface_field=surface_field, conv_a=conv_a, conv_b=conv_b, norm_gain=norm_gain, qkv_weight=qkv_weight, out_weight=out_weight)


def convolve(values_in, weight):
    beside_all = jnp.pad(values_in, ((0, 0), (1, 1), (0, 0)), mode='wrap')
    beside_all = jnp.pad(beside_all, ((1, 1), (0, 0), (0, 0)))
    return lax.conv_general_dilated(beside_all[None], weight, (1, 1), 'VALID', dimension_numbers=('NHWC', 'HWIO', 'NHWC'), preferred_element_type=jnp.float32)[0]

def average_pool(values_in):
    rows_in, cols_in, chans_in = values_in.shape
    return values_in.reshape(rows_in // 2, 2, cols_in // 2, 2, chans_in).mean(axis=(1, 3))

def layer_norm(tokens_flat, norm_gain):
    centred = tokens_flat - lax.optimization_barrier(jnp.mean(tokens_flat, axis=-1, keepdims=True))
    spread = lax.optimization_barrier(jnp.mean(centred * centred, axis=-1, keepdims=True))
    return centred * lax.rsqrt(spread + 0.01) * norm_gain

def softmax_rows(scores):
    maxima = lax.optimization_barrier(jnp.max(scores, axis=-1, keepdims=True))
    raised = jnp.exp(scores - maxima)
    return raised / lax.optimization_barrier(jnp.sum(raised, axis=-1, keepdims=True))

def reference(surface_field, conv_a, conv_b, norm_gain, qkv_weight, out_weight):
    first_out = jax.nn.silu(convolve(surface_field, conv_a))
    pooled_first = average_pool(first_out).astype(jnp.bfloat16)
    second_out = jax.nn.silu(convolve(pooled_first, conv_b))
    pooled_second = average_pool(second_out)
    rows_out, cols_out = (pooled_second.shape[0], pooled_second.shape[1])
    token_count = rows_out * cols_out
    tokens_flat = pooled_second.reshape(token_count, CB)
    normed = layer_norm(tokens_flat, norm_gain).astype(jnp.bfloat16)
    projected = jnp.dot(normed, qkv_weight, preferred_element_type=jnp.float32).astype(jnp.bfloat16)
    per_head = projected.reshape(token_count, 3, HEADS, HEAD_DIM).transpose(1, 2, 0, 3)
    block_rows = math.gcd(token_count, 512)
    score_scale = HEAD_DIM ** (-0.5)

    def one_head(triple):
        queries, keys_here, values_here = triple

        def one_block(query_block):
            scores = jnp.dot(query_block, keys_here.T, preferred_element_type=jnp.float32) * score_scale
            weights = softmax_rows(scores).astype(jnp.bfloat16)
            return jnp.dot(weights, values_here, preferred_element_type=jnp.float32).astype(jnp.bfloat16)
        blocks = lax.map(one_block, queries.reshape(token_count // block_rows, block_rows, HEAD_DIM))
        return blocks.reshape(token_count, HEAD_DIM)
    attended = lax.map(one_head, (per_head[0], per_head[1], per_head[2]))
    attended = attended.transpose(1, 0, 2).reshape(token_count, HEADS * HEAD_DIM)
    mixed_out = tokens_flat + jnp.dot(attended, out_weight, preferred_element_type=jnp.float32)
    return mixed_out.reshape(rows_out, cols_out, CB).astype(jnp.bfloat16)
```

```python
import functools

import jax
import jax.numpy as jnp
from jax import lax
from jax.experimental import pallas as pl
from jax.experimental.pallas import tpu as pltpu
from jax.sharding import PartitionSpec as P

CB = 512
HEADS = 16
HEAD_DIM = 64
CHUNKS = 2


def with_halo(block, sides, width):
    for axis, dim in sides:
        count = lax.axis_size(axis)
        forward = [(i, i + 1) for i in range(count - 1)]
        forward.append((count - 1, 0))
        backward = [(target, source) for source, target in forward]
        low = lax.ppermute(
            lax.slice_in_dim(block, block.shape[dim] - width, None, axis=dim), axis, forward
        )
        high = lax.ppermute(lax.slice_in_dim(block, 0, width, axis=dim), axis, backward)
        block = jnp.concatenate([low, block, high], axis=dim)
    return block


def partner_2(value, axis, distance):
    mask = 2**distance
    pairs = [(source, source ^ mask) for source in range(lax.axis_size(axis))]
    return lax.ppermute(value, axis, pairs)


def convolve(values_in, weight):
    return lax.conv_general_dilated(
        values_in[None],
        weight,
        (1, 1),
        "VALID",
        dimension_numbers=("NHWC", "HWIO", "NHWC"),
        preferred_element_type=jnp.float32,
    )[0]


def average_pool(values_in):
    rows_in, cols_in, chans_in = values_in.shape
    return values_in.reshape(rows_in // 2, 2, cols_in // 2, 2, chans_in).mean(axis=(1, 3))


def layer_norm(tokens_flat, norm_gain):
    centred = tokens_flat - jnp.mean(tokens_flat, axis=-1, keepdims=True)
    spread = jnp.mean(centred * centred, axis=-1, keepdims=True)
    return centred * lax.rsqrt(spread + 0.01) * norm_gain


def softmax_rows(scores):
    maxima = jnp.max(scores, axis=-1, keepdims=True)
    raised = jnp.exp(scores - maxima)
    return raised / jnp.sum(raised, axis=-1, keepdims=True)


def keep_rows(values_in, rows_here, lat_count, lat_where, margin):
    first_row = lat_where * rows_here - margin
    rowpos = first_row + jnp.arange(values_in.shape[0], dtype=jnp.int32)
    inside = (rowpos >= 0) & (rowpos < rows_here * lat_count)
    return jnp.where(inside[:, None, None], values_in, jnp.zeros((), values_in.dtype))


def body(surface_field, conv_a, conv_b, norm_gain, qkv_weight, out_weight):
    lon_count = lax.axis_size("lon")
    lat_count = lax.axis_size("lat")
    lat_where = lax.axis_index("lat")
    rows_here = surface_field.shape[0]
    padded_field = with_halo(surface_field, (("lon", 1), ("lat", 0)), 1)
    padded_field = keep_rows(padded_field, rows_here, lat_count, lat_where, 1)
    first_out = jax.nn.silu(convolve(padded_field, conv_a))
    pooled_first = average_pool(first_out).astype(jnp.bfloat16)
    ready_rows = with_halo(pooled_first, (("lon", 1), ("lat", 0)), 1)
    ready_rows = keep_rows(ready_rows, rows_here // 2, lat_count, lat_where, 1)
    second_out = jax.nn.silu(convolve(ready_rows, conv_b))
    pooled_second = average_pool(second_out)
    tok_rows, tok_cols = (pooled_second.shape[0], pooled_second.shape[1])
    local_tokens = tok_rows * tok_cols
    tokens_flat = pooled_second.reshape(local_tokens, CB)
    normed = layer_norm(tokens_flat, norm_gain).astype(jnp.bfloat16)
    projected = jnp.dot(normed, qkv_weight, preferred_element_type=jnp.float32).astype(jnp.bfloat16)
    residues = max(1, lon_count // HEADS)
    groups = lon_count // residues
    per_slot = HEADS // groups
    per_residue = local_tokens // residues
    arranged = projected.reshape(per_residue, residues, 3, groups, per_slot, HEAD_DIM)
    outgoing = arranged.transpose(2, 1, 3, 4, 0, 5).reshape(
        3, lon_count, per_slot, per_residue, HEAD_DIM
    )
    swap_bits = list(range(groups.bit_length() - 1, lon_count.bit_length() - 1))
    arrived = lax.all_to_all(outgoing, "lon", split_axis=1, concat_axis=3, tiled=True)
    queries = arrived[0, 0]
    keys_vals = arrived[1:, 0]
    for bit_pos in swap_bits:
        partner = partner_2(keys_vals, "lon", bit_pos)
        keys_vals = jnp.concatenate([keys_vals, partner], axis=2)
    for bit_pos in range(lat_count.bit_length() - 1):
        partner = partner_2(keys_vals, "lat", bit_pos)
        keys_vals = jnp.concatenate([keys_vals, partner], axis=2)
    score_scale = HEAD_DIM ** (-0.5)
    scores = (
        jnp.einsum("hqd,hkd->hqk", queries, keys_vals[0], preferred_element_type=jnp.float32)
        * score_scale
    )
    weights = softmax_rows(scores).astype(jnp.bfloat16)
    head_out = jnp.einsum(
        "hqk,hkd->hqd", weights, keys_vals[1], preferred_element_type=jnp.float32
    ).astype(jnp.bfloat16)
    returned = lax.all_to_all(head_out[None], "lon", split_axis=2, concat_axis=0, tiled=True)
    attended = returned.reshape(residues, groups, per_slot, per_residue, HEAD_DIM).transpose(
        3, 0, 1, 2, 4
    )
    attended = attended.reshape(local_tokens, HEADS * HEAD_DIM)
    mixed_out = tokens_flat + jnp.dot(attended, out_weight, preferred_element_type=jnp.float32)
    return mixed_out.reshape(tok_rows, tok_cols, CB).astype(jnp.bfloat16)


def roll_rows(values, amount):
    count = values.shape[0]
    moved = pltpu.roll(values, amount % count, 0)
    rowpos = lax.broadcasted_iota(jnp.int32, values.shape, 0)
    edge = 0 if amount == 1 else count - 1
    return jnp.where(rowpos == edge, jnp.zeros_like(moved), moved)


def silu(v):
    return v / (1.0 + jnp.exp(-v))


def fused_kernel(
    n, cols, toks, heads, hdim,
    x_hbm, wa_hbm, wb_hbm, gain_hbm, wqkv_hbm, wo_hbm, out_ref,
    x_v, wa, wb, wqkv, wo, gain_ref, xf, xs, edge_out, edge_in, ps, pedge_out, pedge_in,
    gat, keys, vals, qmask, att,
    load_sem, halo_send, halo_recv, z_send, far_send, x_send, c_send, recv,
):
    width = heads * hdim
    me = lax.axis_index("lon")
    core, x_at, z_at = me % 2, (me // 2) % 2, me // 4
    zn = n // 4
    left, right = (me + n - 1) % n, (me + 1) % n
    other_core = me + 1 - 2 * core
    other_x = me + 2 - 4 * x_at
    has_up, has_dn = z_at < zn - 1, z_at > 0

    loads = [
        pltpu.make_async_copy(s, d, load_sem.at[i])
        for i, (s, d) in enumerate(
            ((x_hbm, x_v), (wa_hbm, wa), (wb_hbm, wb), (wqkv_hbm, wqkv), (wo_hbm, wo), (gain_hbm, gain_ref))
        )
    ]
    for c in loads:
        c.start()

    barrier = pltpu.get_barrier_semaphore()

    def greet(dev):
        pl.semaphore_signal(barrier, inc=1, device_id={"lon": dev})

    for dev in (left, right, other_core, other_x):
        greet(dev)

    @pl.when(has_up)
    def _():
        greet(me + 4)

    @pl.when(has_dn)
    def _():
        greet(me - 4)

    ends = jnp.where(has_up, 1, 0) + jnp.where(has_dn, 1, 0)
    for d in range(3, zn):
        far_up, far_dn = z_at + d < zn, z_at - d >= 0
        ends = ends + jnp.where(far_up, 1, 0) + jnp.where(far_dn, 1, 0)

        @pl.when(far_up)
        def _(d=d):
            greet(me + 4 * d)

        @pl.when(far_dn)
        def _(d=d):
            greet(me - 4 * d)

    loads[0].wait()
    srows = x_v.shape[0] // cols // 4
    step = 4 * cols
    halves = xf.shape[0]
    for h in range(halves):
        lanes = slice(128 * h, 128 * h + 128)
        xf[h, 0:cols, :] = jnp.zeros((cols, 128), jnp.float32)
        xf[h, cols + x_v.shape[0] :, :] = jnp.zeros((cols, 128), jnp.float32)
        xf[h, cols : cols + x_v.shape[0], :] = x_v[:, lanes].astype(jnp.float32)

    def pick(k, j):
        parts = [
            xf[h, pl.ds(cols + k * cols + j, srows, stride=step), :] for h in range(halves)
        ]
        return jnp.concatenate(parts, axis=1).astype(jnp.bfloat16)

    for side, j in ((0, 0), (1, cols - 1)):
        for k in range(4):
            edge_out[side, k] = pick(k, j)
    pl.semaphore_wait(barrier, 4 + ends)

    def halo(level, src, dst):
        return [
            pltpu.make_async_remote_copy(
                src_ref=src.at[side],
                dst_ref=dst.at[1 - side],
                send_sem=halo_send.at[2 * level + side],
                recv_sem=halo_recv.at[2 * level + 1 - side],
                device_id={"lon": dev},
            )
            for side, dev in ((0, left), (1, right))
        ]

    first = halo(0, edge_out, edge_in)
    for c in first:
        c.start()
    for j in range(cols):
        for k in range(-1, 5):
            xs[k + 1, j + 1] = pick(k, j)

    pcols = cols // 2

    def conv_first(jp):
        taps = [
            xs[a : a + 4, 2 * jp + b : 2 * jp + b + 2].reshape(8 * srows, xs.shape[-1])
            for a in range(3)
            for b in range(3)
        ]
        y = silu(
            jnp.dot(jnp.concatenate(taps, axis=1), wa[...], preferred_element_type=jnp.float32)
        )
        y = y.reshape(4, 2, srows, y.shape[-1])
        even = (y[0, 0] + y[0, 1] + y[1, 0] + y[1, 1]) * 0.25
        odd = (y[2, 0] + y[2, 1] + y[3, 0] + y[3, 1]) * 0.25
        return even, odd

    def put_pooled(at, even, odd):
        ps[0, at] = roll_rows(odd, 1).astype(jnp.bfloat16)
        ps[1, at] = even.astype(jnp.bfloat16)
        ps[2, at] = odd.astype(jnp.bfloat16)
        ps[3, at] = roll_rows(even, -1).astype(jnp.bfloat16)

    loads[1].wait()
    for jp in range(1, pcols - 1):
        put_pooled(jp + 1, *conv_first(jp))

    for c in first:
        c.wait()
    for side, at in ((0, 0), (1, cols + 1)):
        for k in range(4):
            xs[k + 1, at] = edge_in[side, k]
        xs[0, at] = roll_rows(edge_in[side, 3].astype(jnp.float32), 1).astype(jnp.bfloat16)
        xs[5, at] = roll_rows(edge_in[side, 0].astype(jnp.float32), -1).astype(jnp.bfloat16)
    second = halo(1, pedge_out, pedge_in)
    for side, jp in ((0, 0), (1, pcols - 1)):
        even, odd = conv_first(jp)
        pedge_out[side, 0] = even.astype(jnp.bfloat16)
        pedge_out[side, 1] = odd.astype(jnp.bfloat16)
        put_pooled(jp + 1, even, odd)
        second[side].start()

    def conv_second(pieces):
        z = silu(jnp.dot(pieces, wb[...], preferred_element_type=jnp.float32))
        return z.reshape(2, 2, srows, z.shape[-1])

    loads[2].wait()
    loads[5].wait()
    chans = ps.shape[-1]
    inner = conv_second(
        jnp.concatenate(
            [
                ps[a : a + 2, 1 + b : 3 + b].reshape(4 * srows, chans)
                for a in range(3)
                for b in range(3)
            ],
            axis=1,
        )
    )
    for c in second:
        c.wait()
    for side, at in ((0, 0), (1, pcols + 1)):
        put_pooled(
            at,
            pedge_in[side, 0].astype(jnp.float32),
            pedge_in[side, 1].astype(jnp.float32),
        )
    outer = conv_second(
        jnp.concatenate(
            [
                jnp.concatenate(
                    [
                        ps[a : a + 2, b].reshape(2 * srows, chans),
                        ps[a : a + 2, pcols - 1 + b].reshape(2 * srows, chans),
                    ],
                    axis=0,
                )
                for a in range(3)
                for b in range(3)
            ],
            axis=1,
        )
    )
    tokens = jnp.concatenate(
        [
            (inner[0, side] + inner[1, side] + outer[side, 0] + outer[side, 1]) * 0.25
            for side in range(2)
        ],
        axis=0,
    )
    centred = tokens - jnp.mean(tokens, axis=-1, keepdims=True)
    spread = jnp.mean(centred * centred, axis=-1, keepdims=True)
    normed = (centred * lax.rsqrt(spread + 0.01) * gain_ref[...]).astype(jnp.bfloat16)
    chunks = gat.shape[1]
    gat[me] = normed.reshape(gat.shape[1:])
    sent = []

    def go(cond, *made):
        copy = functools.partial(*made)
        sent.append((cond, copy))
        if cond is None:
            copy().start()
        else:
            pl.when(cond)(lambda: copy().start())

    def send(block, ch, dev, sem):
        return pltpu.make_async_remote_copy(
            src_ref=gat.at[block, ch],
            dst_ref=gat.at[block, ch],
            send_sem=sem,
            recv_sem=recv.at[block, ch],
            device_id={"lon": dev},
        )

    def along(block, ch, sign):
        return send(block, ch, me + 4 * sign, z_send.at[(1 - sign) // 2, block // 4, ch])

    def far(block, ch, sign, d):
        return send(block, ch, me + 4 * sign * d, far_send.at[(1 - sign) // 2, d, ch])

    def across(block, ch):
        return send(block, ch, other_x, x_send.at[block // 4, ch])

    def beside(block, ch):
        return send(block, ch, other_core, c_send.at[block // 2, ch])

    def arrived(block, ch):
        send(block, ch, other_core, c_send.at[0, 0]).wait_recv()

    def rows_at(d):
        if d == 0:
            return [(0, None, z_at)]
        return [
            (sign, (z_at + sign * d >= 0) & (z_at + sign * d < zn), z_at + sign * d)
            for sign in (-1, 1)
        ]

    for ch in range(chunks):
        for d in range(zn - 1, 2, -1):
            for sign, ok, _ in rows_at(d):
                go(ok, far, me, ch, sign, d)
        go(has_up, along, me, ch, 1)
        go(has_dn, along, me, ch, -1)
        go(None, across, me, ch)
        go(None, beside, me, ch)

    loads[3].wait()
    group = 4 * hdim
    queries = jnp.dot(normed, wqkv[:, 0:width], preferred_element_type=jnp.float32)
    queries = queries.astype(jnp.bfloat16) * jnp.bfloat16(hdim**-0.5)
    lane_head = (lax.broadcasted_iota(jnp.int32, queries.shape, 1) % group) // hdim
    for a in range(4):
        qmask[a * toks : (a + 1) * toks, :] = jnp.where(
            lane_head == a, queries, jnp.zeros_like(queries)
        )

    def line(d):
        for ch in range(chunks):
            for sign, ok, row in rows_at(d):
                block = row * 4 + me % 4
                pl.when(ok)(functools.partial(arrived, block, ch))
                if d == 1:
                    go(ok & (has_up if sign < 0 else has_dn), along, block, ch, -sign)
                go(ok, across, block, ch)
                go(ok, beside, block, ch)

    def pass_on(d):
        for ch in range(chunks):
            for _, ok, row in rows_at(d):
                block = row * 4 + other_x % 4
                if ok is None:
                    arrived(block, ch)
                else:
                    pl.when(ok)(functools.partial(arrived, block, ch))
                go(ok, beside, block, ch)

    def project(row):
        for ch in range(chunks):
            arrived(row * 4 + other_core % 4, ch)
            arrived(row * 4 + 2 * (1 - x_at) + 1 - core, ch)
        have = gat[pl.ds(row * 4, 4)].reshape(4 * toks, chans)
        kv = jnp.dot(have, wqkv[:, width:], preferred_element_type=jnp.float32)
        kv = kv.astype(jnp.bfloat16)
        keys[row] = kv[:, 0:width]
        vals[row] = kv[:, width:]

    def project_both(d):
        @pl.loop(0, 2)
        def _(t):
            row = z_at + d * (2 * t - 1)

            @pl.when((row >= 0) & (row < zn))
            def _():
                project(row)

    if zn > 1:
        line(1)
    pass_on(0)
    project(z_at)
    for d in range(1, zn):
        if d == 1:
            for later in range(2, zn):
                line(later)
        pass_on(d)
        if d > 1:
            project_both(d - 1)
    if zn > 1:
        project_both(zn - 1)

    for g in range(heads // 4):
        lanes = slice(g * group, (g + 1) * group)
        scores = lax.dot_general(
            qmask[:, lanes],
            keys[:, :, lanes].reshape(n * toks, group),
            (((1,), (1,)), ((), ())),
            preferred_element_type=jnp.float32,
        )
        raised = jnp.exp(scores - jnp.max(scores, axis=-1, keepdims=True))
        total = jnp.sum(raised, axis=-1, keepdims=True)
        weights = (raised * (1.0 / total)).astype(jnp.bfloat16)
        mixed = jnp.dot(
            weights,
            vals[:, :, lanes].reshape(n * toks, group),
            preferred_element_type=jnp.float32,
        )
        heads_at = lax.broadcasted_iota(jnp.int32, (toks, group), 1) // hdim
        got = mixed[0:toks]
        for a in range(1, 4):
            got = jnp.where(heads_at == a, mixed[a * toks : (a + 1) * toks], got)
        att[:, lanes] = got.astype(jnp.bfloat16)

    loads[4].wait()
    final = tokens + jnp.dot(att[...], wo[...], preferred_element_type=jnp.float32)
    out_ref[...] = final.reshape(out_ref.shape).astype(jnp.bfloat16)

    for cond, copy in sent:
        if cond is None:
            copy().wait_send()
        else:
            pl.when(cond)(lambda copy=copy: copy().wait_send())


def fast_body(n, surface_field, conv_a, conv_b, norm_gain, qkv_weight, out_weight):
    rows, cols, chans_in = surface_field.shape
    chans = conv_a.shape[-1]
    srows, tcols = rows // 4, cols // 4
    toks = srows * tcols
    width = out_weight.shape[0]
    heads, zn = width // HEAD_DIM, n // 4
    bf16, f32 = jnp.bfloat16, jnp.float32
    vm, anyw = pl.BlockSpec(memory_space=pltpu.VMEM), pl.BlockSpec(memory_space=pltpu.HBM)
    out = pl.pallas_call(
        functools.partial(fused_kernel, n, cols, toks, heads, HEAD_DIM),
        out_shape=pltpu.VMEM((tcols, srows, chans), bf16),
        in_specs=[anyw] * 6,
        out_specs=vm,
        scratch_shapes=[
            pltpu.VMEM((rows * cols, chans_in), bf16),
            pltpu.VMEM((9 * chans_in, chans), bf16),
            pltpu.VMEM((9 * chans, chans), bf16),
            pltpu.VMEM(qkv_weight.shape, bf16),
            pltpu.VMEM(out_weight.shape, bf16),
            pltpu.VMEM((1, chans), f32),
            pltpu.VMEM((chans_in // 128, (rows + 2) * cols, 128), f32),
            pltpu.VMEM((6, cols + 2, srows, chans_in), bf16),
            pltpu.VMEM((2, 4, srows, chans_in), bf16),
            pltpu.VMEM((2, 4, srows, chans_in), bf16),
            pltpu.VMEM((4, cols // 2 + 2, srows, chans), bf16),
            pltpu.VMEM((2, 2, srows, chans), bf16),
            pltpu.VMEM((2, 2, srows, chans), bf16),
            pltpu.VMEM((n, CHUNKS, toks // CHUNKS, chans), bf16),
            pltpu.VMEM((zn, 4 * toks, width), bf16),
            pltpu.VMEM((zn, 4 * toks, width), bf16),
            pltpu.VMEM((4 * toks, width), bf16),
            pltpu.VMEM((toks, width), bf16),
            pltpu.SemaphoreType.DMA((6,)),
            pltpu.SemaphoreType.DMA((4,)),
            pltpu.SemaphoreType.DMA((4,)),
            pltpu.SemaphoreType.DMA((2, zn, CHUNKS)),
            pltpu.SemaphoreType.DMA((2, zn, CHUNKS)),
            pltpu.SemaphoreType.DMA((zn, CHUNKS)),
            pltpu.SemaphoreType.DMA((2 * zn, CHUNKS)),
            pltpu.SemaphoreType.DMA((n, CHUNKS)),
        ],
        compiler_params=pltpu.CompilerParams(
            collective_id=0, has_side_effects=True, vmem_limit_bytes=48 * 2**20
        ),
    )(
        *(
            pltpu.with_memory_space_constraint(v, pltpu.HBM)
            for v in (
                surface_field.reshape(rows * cols, chans_in),
                conv_a.reshape(9 * chans_in, chans),
                conv_b.reshape(9 * chans, chans),
                norm_gain.reshape(1, chans),
                qkv_weight,
                out_weight,
            )
        )
    )
    return out.transpose(1, 0, 2)


def solution(mesh):
    n = mesh.shape["lon"]
    plain = mesh.shape["lat"] > 1 or n % 4 or n < 4 or n > 16
    run = body if plain else functools.partial(fast_body, n)
    in_specs = (P(("grp", "lat"), "lon", None), P(), P(), P(), P(), P())
    out_specs = P(("grp", "lat"), "lon", None)
    return jax.shard_map(run, mesh=mesh, in_specs=in_specs, out_specs=out_specs, check_vma=False)
```

```python
import functools

import jax
import jax.numpy as jnp
from jax import lax
from jax.experimental import pallas as pl
from jax.experimental.pallas import tpu as pltpu
from jax.sharding import PartitionSpec as P

CB = 512
HEADS = 16
HEAD_DIM = 64
CHUNKS = 2


def with_halo(block, sides, width):
    for axis, dim in sides:
        count = lax.axis_size(axis)
        forward = [(i, i + 1) for i in range(count - 1)]
        forward.append((count - 1, 0))
        backward = [(target, source) for source, target in forward]
        low = lax.ppermute(
            lax.slice_in_dim(block, block.shape[dim] - width, None, axis=dim), axis, forward
        )
        high = lax.ppermute(lax.slice_in_dim(block, 0, width, axis=dim), axis, backward)
        block = jnp.concatenate([low, block, high], axis=dim)
    return block


def partner_2(value, axis, distance):
    mask = 2**distance
    pairs = [(source, source ^ mask) for source in range(lax.axis_size(axis))]
    return lax.ppermute(value, axis, pairs)


def convolve(values_in, weight):
    return lax.conv_general_dilated(
        values_in[None],
        weight,
        (1, 1),
        "VALID",
        dimension_numbers=("NHWC", "HWIO", "NHWC"),
        preferred_element_type=jnp.float32,
    )[0]


def average_pool(values_in):
    rows_in, cols_in, chans_in = values_in.shape
    return values_in.reshape(rows_in // 2, 2, cols_in // 2, 2, chans_in).mean(axis=(1, 3))


def layer_norm(tokens_flat, norm_gain):
    centred = tokens_flat - jnp.mean(tokens_flat, axis=-1, keepdims=True)
    spread = jnp.mean(centred * centred, axis=-1, keepdims=True)
    return centred * lax.rsqrt(spread + 0.01) * norm_gain


def softmax_rows(scores):
    maxima = jnp.max(scores, axis=-1, keepdims=True)
    raised = jnp.exp(scores - maxima)
    return raised / jnp.sum(raised, axis=-1, keepdims=True)


def keep_rows(values_in, rows_here, lat_count, lat_where, margin):
    first_row = lat_where * rows_here - margin
    rowpos = first_row + jnp.arange(values_in.shape[0], dtype=jnp.int32)
    inside = (rowpos >= 0) & (rowpos < rows_here * lat_count)
    return jnp.where(inside[:, None, None], values_in, jnp.zeros((), values_in.dtype))


def body(surface_field, conv_a, conv_b, norm_gain, qkv_weight, out_weight):
    lon_count = lax.axis_size("lon")
    lat_count = lax.axis_size("lat")
    lat_where = lax.axis_index("lat")
    rows_here = surface_field.shape[0]
    padded_field = with_halo(surface_field, (("lon", 1), ("lat", 0)), 1)
    padded_field = keep_rows(padded_field, rows_here, lat_count, lat_where, 1)
    first_out = jax.nn.silu(convolve(padded_field, conv_a))
    pooled_first = average_pool(first_out).astype(jnp.bfloat16)
    ready_rows = with_halo(pooled_first, (("lon", 1), ("lat", 0)), 1)
    ready_rows = keep_rows(ready_rows, rows_here // 2, lat_count, lat_where, 1)
    second_out = jax.nn.silu(convolve(ready_rows, conv_b))
    pooled_second = average_pool(second_out)
    tok_rows, tok_cols = (pooled_second.shape[0], pooled_second.shape[1])
    local_tokens = tok_rows * tok_cols
    tokens_flat = pooled_second.reshape(local_tokens, CB)
    normed = layer_norm(tokens_flat, norm_gain).astype(jnp.bfloat16)
    projected = jnp.dot(normed, qkv_weight, preferred_element_type=jnp.float32).astype(jnp.bfloat16)
    residues = max(1, lon_count // HEADS)
    groups = lon_count // residues
    per_slot = HEADS // groups
    per_residue = local_tokens // residues
    arranged = projected.reshape(per_residue, residues, 3, groups, per_slot, HEAD_DIM)
    outgoing = arranged.transpose(2, 1, 3, 4, 0, 5).reshape(
        3, lon_count, per_slot, per_residue, HEAD_DIM
    )
    swap_bits = list(range(groups.bit_length() - 1, lon_count.bit_length() - 1))
    arrived = lax.all_to_all(outgoing, "lon", split_axis=1, concat_axis=3, tiled=True)
    queries = arrived[0, 0]
    keys_vals = arrived[1:, 0]
    for bit_pos in swap_bits:
        partner = partner_2(keys_vals, "lon", bit_pos)
        keys_vals = jnp.concatenate([keys_vals, partner], axis=2)
    for bit_pos in range(lat_count.bit_length() - 1):
        partner = partner_2(keys_vals, "lat", bit_pos)
        keys_vals = jnp.concatenate([keys_vals, partner], axis=2)
    score_scale = HEAD_DIM ** (-0.5)
    scores = (
        jnp.einsum("hqd,hkd->hqk", queries, keys_vals[0], preferred_element_type=jnp.float32)
        * score_scale
    )
    weights = softmax_rows(scores).astype(jnp.bfloat16)
    head_out = jnp.einsum(
        "hqk,hkd->hqd", weights, keys_vals[1], preferred_element_type=jnp.float32
    ).astype(jnp.bfloat16)
    returned = lax.all_to_all(head_out[None], "lon", split_axis=2, concat_axis=0, tiled=True)
    attended = returned.reshape(residues, groups, per_slot, per_residue, HEAD_DIM).transpose(
        3, 0, 1, 2, 4
    )
    attended = attended.reshape(local_tokens, HEADS * HEAD_DIM)
    mixed_out = tokens_flat + jnp.dot(attended, out_weight, preferred_element_type=jnp.float32)
    return mixed_out.reshape(tok_rows, tok_cols, CB).astype(jnp.bfloat16)


def roll_rows(values, amount):
    count = values.shape[0]
    moved = pltpu.roll(values, amount % count, 0)
    rowpos = lax.broadcasted_iota(jnp.int32, values.shape, 0)
    edge = 0 if amount == 1 else count - 1
    return jnp.where(rowpos == edge, jnp.zeros_like(moved), moved)


def silu(v):
    half = 0.5 * v
    return half + half * jnp.tanh(half)


def fused_kernel(
    n, cols, toks, heads, hdim,
    x_hbm, wa_hbm, wb_hbm, gain_hbm, wqkv_hbm, wo_hbm, out_ref,
    x_v, wa, wb, wqkv, wo, gain_ref, xs, edge_in, ps, pedge_out, pedge_in,
    gat, sums, totals, peaks, qmask, att,
    load_sem, near_ok, halo_send, halo_recv, block_send, block_recv, side_recv,
):
    width = heads * hdim
    me = lax.axis_index("lon")
    core, x_at, z_at = me % 2, (me // 2) % 2, me // 4
    other_core = me + 1 - 2 * core
    other_x = me + 2 - 4 * x_at
    beyond = (me + n - 1 + 2 * core) % n
    wraps = me // (n - 1) + (n - 1 - me) // (n - 1)
    first, last = me == 0, me == n - 1
    wrap, inner = first | last, (me > 0) & (me < n - 1)
    near, two = z_at + 1 - 2 * (z_at // 2), (z_at + 2) % 4
    rest = (near + 2) % 4
    ends = z_at // 3 + (3 - z_at) // 3
    middle, edge = (z_at > 0) & (z_at < 3), (z_at == 0) | (z_at == 3)
    own, mate = me % 4, other_x % 4

    loads = [
        pltpu.make_async_copy(s, d, load_sem.at[i])
        for i, (s, d) in enumerate(
            (
                (x_hbm, x_v), (wa_hbm, wa), (wb_hbm, wb),
                (gain_hbm, gain_ref), (wqkv_hbm, wqkv), (wo_hbm, wo),
            )
        )
    ]
    for c in loads:
        c.start()

    barrier = pltpu.get_barrier_semaphore()

    def greet(dev):
        pl.semaphore_signal(barrier, inc=1, device_id={"lon": dev})

    for dev in (beyond, other_core, other_x, two * 4 + own, near * 4 + own, near * 4 + mate):
        greet(dev)

    @pl.when(middle)
    def _():
        greet(rest * 4 + own)
        greet(rest * 4 + mate)

    greeted = 8 - 2 * ends

    srows = x_v.shape[0] // cols // 4
    span = 32 * cols
    row = lax.broadcasted_iota(jnp.int32, (span, span), 0)
    col = lax.broadcasted_iota(jnp.int32, (span, span), 1)
    source = (4 * (row % 8) + row // (8 * cols)) * cols + (row // 8) % cols
    order = jnp.where(col == source, 1.0, 0.0).astype(jnp.bfloat16)
    loads[0].wait()
    turned = [
        jnp.dot(order, x_v[at : at + span, :], preferred_element_type=jnp.float32)
        for at in range(0, x_v.shape[0], span)
    ]

    def column(k, j):
        at = (k * cols + j) * 8
        return jnp.concatenate([t[at : at + 8] for t in turned], axis=0)

    for j in range(cols):
        for k in range(4):
            xs[k + 1, j + 3] = column(k, j).astype(jnp.bfloat16)

    def halo(i, k, src, dst, dev):
        return pltpu.make_async_remote_copy(
            src_ref=src,
            dst_ref=dst,
            send_sem=halo_send.at[k],
            recv_sem=halo_recv.at[i],
            device_id={"lon": dev},
        )

    def edge_column(j):
        return xs.at[pl.ds(1, 4), j + 3]

    by_near = halo(3, 0, edge_column((1 - core) * (cols - 1)), edge_in.at[3], other_core)
    by_far = [
        halo(
            min(i, 1), 0, edge_column(core * (cols - 1) + (1 - 2 * core) * i), edge_in.at[i], beyond
        )
        for i in range(3)
    ]
    by_near_2 = halo(4, 1, pedge_out.at[0], pedge_in.at[0], other_core)
    by_far_2 = halo(2, 1, pedge_out.at[1], pedge_in.at[1], beyond)

    @pl.when(me > 0)
    def _():
        pl.semaphore_wait(barrier, greeted)

    @pl.when(first)
    def _():
        pl.semaphore_wait(near_ok, 1)

    @pl.when(me == 1)
    def _():
        pl.semaphore_signal(near_ok, inc=1, device_id={"lon": other_core})

    @pl.when(me > 0)
    def _():
        by_far[0].start()

    by_near.start()

    @pl.when(last)
    def _():
        by_far[1].start()
        by_far[2].start()

    for j in range(cols):
        xs[0, j + 3] = roll_rows(column(3, j), 1).astype(jnp.bfloat16)
        xs[5, j + 3] = roll_rows(column(0, j), -1).astype(jnp.bfloat16)

    pcols = cols // 2

    def conv_first(*jps):
        taps = [
            jnp.concatenate(
                [
                    xs[a : a + 4, pl.ds(2 * jp + 2 + b, 2)].reshape(8 * srows, xs.shape[-1])
                    for jp in jps
                ],
                axis=0,
            )
            for a in range(3)
            for b in range(3)
        ]
        y = silu(
            jnp.dot(jnp.concatenate(taps, axis=1), wa[...], preferred_element_type=jnp.float32)
        )
        y = y.reshape(len(jps), 4, 2, srows, y.shape[-1])
        return [
            [
                (y[i, k, 0] + y[i, k, 1] + y[i, k + 1, 0] + y[i, k + 1, 1]) * 0.25
                for k in (0, 2)
            ]
            for i in range(len(jps))
        ]

    def put_pooled(at, even, odd):
        ps[0, at] = roll_rows(odd, 1).astype(jnp.bfloat16)
        ps[1, at] = even.astype(jnp.bfloat16)
        ps[2, at] = odd.astype(jnp.bfloat16)
        ps[3, at] = roll_rows(even, -1).astype(jnp.bfloat16)

    def put_edge(side, even, odd):
        pedge_out[side, 0] = even.astype(jnp.bfloat16)
        pedge_out[side, 1] = odd.astype(jnp.bfloat16)

    def put_column(i, at):
        for k in range(4):
            xs[k + 1, at] = edge_in[i, k]
        xs[0, at] = roll_rows(edge_in[i, 3].astype(jnp.float32), 1).astype(jnp.bfloat16)
        xs[5, at] = roll_rows(edge_in[i, 0].astype(jnp.float32), -1).astype(jnp.bfloat16)

    def put_far(i):
        put_column(i, 2 - i + core * (cols + 1 + 2 * i))

    jp_near, jp_far = (1 - core) * (pcols - 1), core * (pcols - 1)
    jp_third = jp_far + wraps * (2 - jp_far)
    jp_fourth = 2 + jp_far - jp_third
    loads[1].wait()
    by_near.wait_recv()
    put_column(3, (1 - core) * (cols + 1) + 2)
    inside, beside_near = conv_first(1, jp_near)
    put_pooled(jp_near + 1, *beside_near)
    put_edge(0, *beside_near)
    put_pooled(2, *inside)
    by_near_2.start()

    @pl.when(first)
    def _():
        pl.semaphore_wait(barrier, greeted)
        for copy in by_far:
            copy.start()

    @pl.when(inner)
    def _():
        by_far[0].wait_recv()
        put_far(0)

    (third,) = conv_first(jp_third)
    put_edge(1, *third)
    put_pooled(jp_third + 1, *third)

    @pl.when(inner)
    def _():
        by_far_2.start()

    @pl.when(wrap)
    def _():
        by_far[0].wait_recv()
        put_far(0)

    def conv_second(pieces):
        z = silu(jnp.dot(pieces, wb[...], preferred_element_type=jnp.float32))
        return z.reshape(2, 2, srows, z.shape[-1])

    loads[2].wait()
    loads[3].wait()
    (fourth,) = conv_first(jp_fourth)
    put_pooled(jp_fourth + 1, *fourth)
    chans = ps.shape[-1]
    inside = conv_second(
        jnp.concatenate(
            [
                ps[a : a + 2, 1 + b : 3 + b].reshape(4 * srows, chans)
                for a in range(3)
                for b in range(3)
            ],
            axis=1,
        )
    )
    by_near_2.wait_recv()
    put_pooled(
        (1 - core) * (pcols + 1),
        pedge_in[0, 0].astype(jnp.float32),
        pedge_in[0, 1].astype(jnp.float32),
    )
    far_at = core * (pcols + 1)

    @pl.when(inner)
    def _():
        by_far_2.wait_recv()
        put_pooled(
            far_at, pedge_in[1, 0].astype(jnp.float32), pedge_in[1, 1].astype(jnp.float32)
        )

    @pl.when(wrap)
    def _():
        both = edge_in.at[pl.ds(1, 2)]
        halo(1, 0, both, both, beyond).wait_recv()
        put_far(1)
        put_far(2)
        put_pooled(far_at, *conv_first(core * (pcols + 1) - 1)[0])

    outer = conv_second(
        jnp.concatenate(
            [
                jnp.concatenate(
                    [
                        ps[a : a + 2, b].reshape(2 * srows, chans),
                        ps[a : a + 2, pcols - 1 + b].reshape(2 * srows, chans),
                    ],
                    axis=0,
                )
                for a in range(3)
                for b in range(3)
            ],
            axis=1,
        )
    )
    tokens = jnp.concatenate(
        [
            (inside[0, side] + inside[1, side] + outer[side, 0] + outer[side, 1]) * 0.25
            for side in range(2)
        ],
        axis=0,
    )
    centred = tokens - jnp.mean(tokens, axis=-1, keepdims=True)
    spread = jnp.mean(centred * centred, axis=-1, keepdims=True)
    normed = (centred * lax.rsqrt(spread + 0.01) * gain_ref[...]).astype(jnp.bfloat16)
    chunks = gat.shape[1]
    gat[me] = normed.reshape(gat.shape[1:])

    def send(block, ch, dev, sem):
        return pltpu.make_async_remote_copy(
            src_ref=gat.at[block, ch],
            dst_ref=gat.at[block, ch],
            send_sem=block_send,
            recv_sem=sem,
            device_id={"lon": dev},
        )

    def go(block, ch, dev):
        send(block, ch, dev, block_recv.at[block // 2, ch]).start()

    def beside(block, ch, unit):
        send(block, ch, other_core, side_recv.at[unit]).start()

    def arrived(block, ch):
        send(block, ch, other_core, block_recv.at[block // 2, ch]).wait_recv()

    for ch in range(chunks):
        go(me, ch, two * 4 + own)
        go(me, ch, other_x)
        beside(me, ch, 0)

    @pl.when(middle)
    def _():
        for ch in range(chunks):
            go(me, ch, rest * 4 + own)

    for ch in range(chunks):
        go(me, ch, near * 4 + mate)
    for ch in range(chunks):
        go(me, ch, near * 4 + own)

    loads[4].wait()
    group = 4 * hdim
    queries = jnp.dot(normed, wqkv[:, 0:width], preferred_element_type=jnp.float32)
    queries = queries.astype(jnp.bfloat16) * jnp.bfloat16(hdim**-0.5)
    lane_head = (lax.broadcasted_iota(jnp.int32, queries.shape, 1) % group) // hdim
    for a in range(4):
        qmask[a * toks : (a + 1) * toks, :] = jnp.where(
            lane_head == a, queries, jnp.zeros_like(queries)
        )
    heads_at = lax.broadcasted_iota(jnp.int32, (toks, group), 1) // hdim

    def by_head(v):
        got = v[0:toks]
        for a in range(1, 4):
            got = jnp.where(heads_at == a, v[a * toks : (a + 1) * toks], got)
        return got

    def attend(unit, chips, start=False, end=False):
        count = len(chips)
        both = gat.at[pl.ds(0, count)]
        pltpu.make_async_remote_copy(
            src_ref=both,
            dst_ref=both,
            send_sem=block_send,
            recv_sem=side_recv.at[unit],
            device_id={"lon": other_core},
        ).wait_recv()
        have = jnp.concatenate(
            [gat[pl.ds(2 * c, 2)].reshape(2 * toks, chans) for c in chips], axis=0
        )
        keys, vals, mixes, norms = {}, {}, {}, {}

        def project(g):
            for held, at in ((keys, width), (vals, 2 * width)):
                at = at + g * group
                made = jnp.dot(have, wqkv[:, at : at + group], preferred_element_type=jnp.float32)
                held[g] = made.astype(jnp.bfloat16)

        def score(g):
            scores = lax.dot_general(
                qmask[:, g * group : (g + 1) * group],
                keys[g],
                (((1,), (1,)), ((), ())),
                preferred_element_type=jnp.float32,
            )
            peak = jnp.max(scores, axis=-1, keepdims=True)
            raised = jnp.exp(scores - peak)
            norms[g] = peak, jnp.sum(raised, axis=-1, keepdims=True)
            mixes[g] = raised.astype(jnp.bfloat16)

        def mix(g):
            lanes = slice(g * group, (g + 1) * group)
            mixed = jnp.dot(mixes[g], vals[g], preferred_element_type=jnp.float32)
            got, peak, total = by_head(mixed), by_head(norms[g][0]), by_head(norms[g][1])
            if not start:
                top = jnp.maximum(peaks[:, lanes], peak)
                was, now = jnp.exp(peaks[:, lanes] - top), jnp.exp(peak - top)
                got = sums[:, lanes] * was + got * now
                total = totals[:, lanes] * was + total * now
                peak = top
            if end:
                att[:, lanes] = (got * (1.0 / total)).astype(jnp.bfloat16)
            else:
                sums[:, lanes], totals[:, lanes], peaks[:, lanes] = got, total, peak

        groups = heads // 4
        for step in range(groups + 2):
            if step < groups:
                project(step)
            if 0 <= step - 1 < groups:
                score(step - 1)
            if 0 <= step - 2 < groups:
                mix(step - 2)

    b_near, b_two, b_rest = near * 4 + own, two * 4 + own, rest * 4 + own
    c_near, c_two, c_rest = near * 4 + mate, two * 4 + mate, rest * 4 + mate

    def take(block, ch, unit, *onward):
        arrived(block, ch)
        for dev in onward:
            go(block, ch, dev)
        beside(block, ch, unit)

    def take_two(ch):
        arrived(b_two, ch)

        @pl.when(middle)
        def _():
            go(b_two, ch, rest * 4 + own)
            go(b_two, ch, rest * 4 + mate)

        go(b_two, ch, other_x)
        beside(b_two, ch, 3 - ends)

    def either(at_middle, at_end):
        return (at_middle + ends * (at_end - at_middle)) // 2

    attend(0, [me // 2], start=True)
    take(other_x, 0, 1)

    @pl.when(edge)
    def _():
        take(b_near, 0, 1, other_x)

    take(other_x, 1, 1)

    @pl.when(edge)
    def _():
        take(b_near, 1, 1, other_x)

    take_two(0)
    take_two(1)

    @pl.when(middle)
    def _():
        for ch in range(chunks):
            take(c_near, ch, 1)
            take(c_rest, ch, 2)
        for ch in range(chunks):
            take(b_rest, ch, 3)
            take(b_near, ch, 2)

    attend(1, [other_x // 2, either(c_near, b_near)])

    @pl.when(edge)
    def _():
        take(c_near, 0, 2)
        take(c_near, 1, 2)
        take(b_rest, 0, 3)

    take(c_two, 0, 4 - ends)
    take(c_two, 1, 4 - ends)

    @pl.when(edge)
    def _():
        take(b_rest, 1, 3)

    attend(2, [either(c_rest, b_two), either(b_near, c_near)])

    @pl.when(edge)
    def _():
        take(c_rest, 0, 4)
        take(c_rest, 1, 4)

    attend(3, [b_rest // 2, either(b_two, c_two)])
    attend(4, [either(c_two, c_rest)], end=True)

    loads[5].wait()
    final = tokens + jnp.dot(att[...], wo[...], preferred_element_type=jnp.float32)
    out_ref[...] = final.reshape(out_ref.shape).astype(jnp.bfloat16)

    def drain(ref, sem):
        pltpu.make_async_remote_copy(
            src_ref=ref,
            dst_ref=ref,
            send_sem=sem,
            recv_sem=halo_recv.at[0],
            device_id={"lon": other_core},
        ).wait_send()

    @pl.when(inner)
    def _():
        drain(edge_in.at[pl.ds(0, 2)], halo_send.at[0])
        drain(pedge_in, halo_send.at[1])

    @pl.when(wrap)
    def _():
        drain(edge_in, halo_send.at[0])
        drain(pedge_in.at[0], halo_send.at[1])

    @pl.when(middle)
    def _():
        drain(gat, block_send)

    @pl.when(edge)
    def _():
        drain(gat.at[pl.ds(0, n - 2)], block_send)


def fast_body(n, surface_field, conv_a, conv_b, norm_gain, qkv_weight, out_weight):
    rows, cols, chans_in = surface_field.shape
    chans = conv_a.shape[-1]
    srows, tcols = rows // 4, cols // 4
    toks = srows * tcols
    width = out_weight.shape[0]
    heads = width // HEAD_DIM
    bf16, f32 = jnp.bfloat16, jnp.float32
    vm, anyw = pl.BlockSpec(memory_space=pltpu.VMEM), pl.BlockSpec(memory_space=pltpu.HBM)
    out = pl.pallas_call(
        functools.partial(fused_kernel, n, cols, toks, heads, HEAD_DIM),
        out_shape=pltpu.VMEM((tcols, srows, chans), bf16),
        in_specs=[anyw] * 6,
        out_specs=vm,
        scratch_shapes=[
            pltpu.VMEM((rows * cols, chans_in), bf16),
            pltpu.VMEM((9 * chans_in, chans), bf16),
            pltpu.VMEM((9 * chans, chans), bf16),
            pltpu.VMEM(qkv_weight.shape, bf16),
            pltpu.VMEM(out_weight.shape, bf16),
            pltpu.VMEM((1, chans), f32),
            pltpu.VMEM((6, cols + 6, srows, chans_in), bf16),
            pltpu.VMEM((4, 4, srows, chans_in), bf16),
            pltpu.VMEM((4, cols // 2 + 2, srows, chans), bf16),
            pltpu.VMEM((2, 2, srows, chans), bf16),
            pltpu.VMEM((2, 2, srows, chans), bf16),
            pltpu.VMEM((n, CHUNKS, toks // CHUNKS, chans), bf16),
            pltpu.VMEM((toks, width), f32),
            pltpu.VMEM((toks, width), f32),
            pltpu.VMEM((toks, width), f32),
            pltpu.VMEM((4 * toks, width), bf16),
            pltpu.VMEM((toks, width), bf16),
            pltpu.SemaphoreType.DMA((6,)),
            pltpu.SemaphoreType.REGULAR,
            pltpu.SemaphoreType.DMA((2,)),
            pltpu.SemaphoreType.DMA((5,)),
            pltpu.SemaphoreType.DMA,
            pltpu.SemaphoreType.DMA((n // 2, CHUNKS)),
            pltpu.SemaphoreType.DMA((5,)),
        ],
        compiler_params=pltpu.CompilerParams(
            collective_id=0, has_side_effects=True, vmem_limit_bytes=48 * 2**20
        ),
    )(
        *(
            pltpu.with_memory_space_constraint(v, pltpu.HBM)
            for v in (
                surface_field.reshape(rows * cols, chans_in),
                conv_a.reshape(9 * chans_in, chans),
                conv_b.reshape(9 * chans, chans),
                norm_gain.reshape(1, chans),
                qkv_weight,
                out_weight,
            )
        )
    )
    return out.transpose(1, 0, 2)


def solution(mesh):
    n = mesh.shape["lon"]
    plain = mesh.shape["lat"] > 1 or n != 16
    run = body if plain else functools.partial(fast_body, n)
    in_specs = (P(("grp", "lat"), "lon", None), P(), P(), P(), P(), P())
    out_specs = P(("grp", "lat"), "lon", None)
    return jax.shard_map(run, mesh=mesh, in_specs=in_specs, out_specs=out_specs, check_vma=False)
```

```python
import functools

import jax
import jax.numpy as jnp
from jax import lax
from jax.experimental import pallas as pl
from jax.experimental.pallas import tpu as pltpu
from jax.sharding import PartitionSpec as P

CB = 512
HEADS = 16
HEAD_DIM = 64
CHUNKS = 2


def with_halo(block, sides, width):
    for axis, dim in sides:
        count = lax.axis_size(axis)
        forward = [(i, i + 1) for i in range(count - 1)]
        forward.append((count - 1, 0))
        backward = [(target, source) for source, target in forward]
        low = lax.ppermute(
            lax.slice_in_dim(block, block.shape[dim] - width, None, axis=dim), axis, forward
        )
        high = lax.ppermute(lax.slice_in_dim(block, 0, width, axis=dim), axis, backward)
        block = jnp.concatenate([low, block, high], axis=dim)
    return block


def partner_2(value, axis, distance):
    mask = 2**distance
    pairs = [(source, source ^ mask) for source in range(lax.axis_size(axis))]
    return lax.ppermute(value, axis, pairs)


def convolve(values_in, weight):
    return lax.conv_general_dilated(
        values_in[None],
        weight,
        (1, 1),
        "VALID",
        dimension_numbers=("NHWC", "HWIO", "NHWC"),
        preferred_element_type=jnp.float32,
    )[0]


def average_pool(values_in):
    rows_in, cols_in, chans_in = values_in.shape
    return values_in.reshape(rows_in // 2, 2, cols_in // 2, 2, chans_in).mean(axis=(1, 3))


def layer_norm(tokens_flat, norm_gain):
    centred = tokens_flat - jnp.mean(tokens_flat, axis=-1, keepdims=True)
    spread = jnp.mean(centred * centred, axis=-1, keepdims=True)
    return centred * lax.rsqrt(spread + 0.01) * norm_gain


def softmax_rows(scores):
    maxima = jnp.max(scores, axis=-1, keepdims=True)
    raised = jnp.exp(scores - maxima)
    return raised / jnp.sum(raised, axis=-1, keepdims=True)


def keep_rows(values_in, rows_here, lat_count, lat_where, margin):
    first_row = lat_where * rows_here - margin
    rowpos = first_row + jnp.arange(values_in.shape[0], dtype=jnp.int32)
    inside = (rowpos >= 0) & (rowpos < rows_here * lat_count)
    return jnp.where(inside[:, None, None], values_in, jnp.zeros((), values_in.dtype))


def body(surface_field, conv_a, conv_b, norm_gain, qkv_weight, out_weight):
    lon_count = lax.axis_size("lon")
    lat_count = lax.axis_size("lat")
    lat_where = lax.axis_index("lat")
    rows_here = surface_field.shape[0]
    padded_field = with_halo(surface_field, (("lon", 1), ("lat", 0)), 1)
    padded_field = keep_rows(padded_field, rows_here, lat_count, lat_where, 1)
    first_out = jax.nn.silu(convolve(padded_field, conv_a))
    pooled_first = average_pool(first_out).astype(jnp.bfloat16)
    ready_rows = with_halo(pooled_first, (("lon", 1), ("lat", 0)), 1)
    ready_rows = keep_rows(ready_rows, rows_here // 2, lat_count, lat_where, 1)
    second_out = jax.nn.silu(convolve(ready_rows, conv_b))
    pooled_second = average_pool(second_out)
    tok_rows, tok_cols = (pooled_second.shape[0], pooled_second.shape[1])
    local_tokens = tok_rows * tok_cols
    tokens_flat = pooled_second.reshape(local_tokens, CB)
    normed = layer_norm(tokens_flat, norm_gain).astype(jnp.bfloat16)
    projected = jnp.dot(normed, qkv_weight, preferred_element_type=jnp.float32).astype(jnp.bfloat16)
    residues = max(1, lon_count // HEADS)
    groups = lon_count // residues
    per_slot = HEADS // groups
    per_residue = local_tokens // residues
    arranged = projected.reshape(per_residue, residues, 3, groups, per_slot, HEAD_DIM)
    outgoing = arranged.transpose(2, 1, 3, 4, 0, 5).reshape(
        3, lon_count, per_slot, per_residue, HEAD_DIM
    )
    swap_bits = list(range(groups.bit_length() - 1, lon_count.bit_length() - 1))
    arrived = lax.all_to_all(outgoing, "lon", split_axis=1, concat_axis=3, tiled=True)
    queries = arrived[0, 0]
    keys_vals = arrived[1:, 0]
    for bit_pos in swap_bits:
        partner = partner_2(keys_vals, "lon", bit_pos)
        keys_vals = jnp.concatenate([keys_vals, partner], axis=2)
    for bit_pos in range(lat_count.bit_length() - 1):
        partner = partner_2(keys_vals, "lat", bit_pos)
        keys_vals = jnp.concatenate([keys_vals, partner], axis=2)
    score_scale = HEAD_DIM ** (-0.5)
    scores = (
        jnp.einsum("hqd,hkd->hqk", queries, keys_vals[0], preferred_element_type=jnp.float32)
        * score_scale
    )
    weights = softmax_rows(scores).astype(jnp.bfloat16)
    head_out = jnp.einsum(
        "hqk,hkd->hqd", weights, keys_vals[1], preferred_element_type=jnp.float32
    ).astype(jnp.bfloat16)
    returned = lax.all_to_all(head_out[None], "lon", split_axis=2, concat_axis=0, tiled=True)
    attended = returned.reshape(residues, groups, per_slot, per_residue, HEAD_DIM).transpose(
        3, 0, 1, 2, 4
    )
    attended = attended.reshape(local_tokens, HEADS * HEAD_DIM)
    mixed_out = tokens_flat + jnp.dot(attended, out_weight, preferred_element_type=jnp.float32)
    return mixed_out.reshape(tok_rows, tok_cols, CB).astype(jnp.bfloat16)


def roll_rows(values, amount):
    count = values.shape[0]
    moved = pltpu.roll(values, amount % count, 0)
    rowpos = lax.broadcasted_iota(jnp.int32, values.shape, 0)
    edge = 0 if amount == 1 else count - 1
    return jnp.where(rowpos == edge, jnp.zeros_like(moved), moved)


def silu(v):
    half = 0.5 * v
    return half + half * jnp.tanh(half)


def fused_kernel(
    n, cols, toks, heads, hdim,
    x_hbm, wa_hbm, wb_hbm, gain_hbm, wqkv_hbm, wo_hbm, out_ref,
    x_v, wa, wb, wqkv, wo, gain_ref, xs, edge_in, ps, pedge_out, pedge_in,
    gat, keys, vals, sums, totals, peaks, qmask, att,
    load_sem, near_ok, told, halo_send, halo_recv, block_send, block_recv, side_recv,
):
    width = heads * hdim
    me = lax.axis_index("lon")
    core, x_at, z_at = me % 2, (me // 2) % 2, me // 4
    other_core = me + 1 - 2 * core
    other_x = me + 2 - 4 * x_at
    beyond = (me + n - 1 + 2 * core) % n
    wraps = me // (n - 1) + (n - 1 - me) // (n - 1)
    first, last = me == 0, me == n - 1
    wrap, inner = first | last, (me > 0) & (me < n - 1)
    near, two = z_at + 1 - 2 * (z_at // 2), (z_at + 2) % 4
    rest = (near + 2) % 4
    ends = z_at // 3 + (3 - z_at) // 3
    middle, edge = (z_at > 0) & (z_at < 3), (z_at == 0) | (z_at == 3)
    own, mate = me % 4, other_x % 4

    loads = [
        pltpu.make_async_copy(s, d, load_sem.at[i])
        for i, (s, d) in enumerate(
            (
                (x_hbm, x_v), (wa_hbm, wa), (wb_hbm, wb),
                (gain_hbm, gain_ref), (wqkv_hbm, wqkv), (wo_hbm, wo),
            )
        )
    ]
    for c in loads:
        c.start()

    barrier = pltpu.get_barrier_semaphore()

    def greet(dev):
        pl.semaphore_signal(barrier, inc=1, device_id={"lon": dev})

    greet(other_core)
    greet(beyond)

    srows = x_v.shape[0] // cols // 4
    span = 32 * cols
    row = lax.broadcasted_iota(jnp.int32, (span, span), 0)
    col = lax.broadcasted_iota(jnp.int32, (span, span), 1)
    source = (4 * (row % 8) + row // (8 * cols)) * cols + (row // 8) % cols
    order = jnp.where(col == source, 1.0, 0.0).astype(jnp.bfloat16)
    loads[0].wait()
    turned = [
        jnp.dot(order, x_v[at : at + span, :], preferred_element_type=jnp.float32)
        for at in range(0, x_v.shape[0], span)
    ]

    def column(k, j):
        at = (k * cols + j) * 8
        return jnp.concatenate([t[at : at + 8] for t in turned], axis=0)

    for j in range(cols):
        for k in range(4):
            xs[k + 1, j + 3] = column(k, j).astype(jnp.bfloat16)

    def halo(i, k, src, dst, dev):
        return pltpu.make_async_remote_copy(
            src_ref=src,
            dst_ref=dst,
            send_sem=halo_send.at[k],
            recv_sem=halo_recv.at[i],
            device_id={"lon": dev},
        )

    def edge_column(j):
        return xs.at[pl.ds(1, 4), j + 3]

    by_near = halo(3, 0, edge_column((1 - core) * (cols - 1)), edge_in.at[3], other_core)
    by_far = [
        halo(
            min(i, 1), 0, edge_column(core * (cols - 1) + (1 - 2 * core) * i), edge_in.at[i], beyond
        )
        for i in range(3)
    ]
    by_near_2 = halo(4, 1, pedge_out.at[0], pedge_in.at[0], other_core)
    by_far_2 = halo(2, 1, pedge_out.at[1], pedge_in.at[1], beyond)

    @pl.when(me > 0)
    def _():
        pl.semaphore_wait(barrier, 2)

    @pl.when(first)
    def _():
        pl.semaphore_wait(near_ok, 1)

    @pl.when(me == 1)
    def _():
        pl.semaphore_signal(near_ok, inc=1, device_id={"lon": other_core})

    @pl.when(me > 0)
    def _():
        by_far[0].start()

    by_near.start()

    @pl.when(last)
    def _():
        by_far[1].start()
        by_far[2].start()

    def tell(level):
        step = 2**level
        for way, dev, real in ((0, me + step, me < n - step), (1, me - step, me >= step)):

            @pl.when(real)
            def _(way=way, dev=dev):
                pl.semaphore_signal(told.at[level, way], inc=1, device_id={"lon": dev})

    def hear(level):
        step = 2**level
        for way, real in ((1, me < n - step), (0, me >= step)):

            @pl.when(real)
            def _(way=way):
                pl.semaphore_wait(told.at[level, way], 1)

    tell(0)
    for j in range(cols):
        xs[0, j + 3] = roll_rows(column(3, j), 1).astype(jnp.bfloat16)
        xs[5, j + 3] = roll_rows(column(0, j), -1).astype(jnp.bfloat16)

    pcols = cols // 2

    def conv_first(*jps):
        taps = [
            jnp.concatenate(
                [
                    xs[a : a + 4, pl.ds(2 * jp + 2 + b, 2)].reshape(8 * srows, xs.shape[-1])
                    for jp in jps
                ],
                axis=0,
            )
            for a in range(3)
            for b in range(3)
        ]
        y = silu(
            jnp.dot(jnp.concatenate(taps, axis=1), wa[...], preferred_element_type=jnp.float32)
        )
        y = y.reshape(len(jps), 4, 2, srows, y.shape[-1])
        return [
            [
                (y[i, k, 0] + y[i, k, 1] + y[i, k + 1, 0] + y[i, k + 1, 1]) * 0.25
                for k in (0, 2)
            ]
            for i in range(len(jps))
        ]

    def put_pooled(at, even, odd):
        ps[0, at] = roll_rows(odd, 1).astype(jnp.bfloat16)
        ps[1, at] = even.astype(jnp.bfloat16)
        ps[2, at] = odd.astype(jnp.bfloat16)
        ps[3, at] = roll_rows(even, -1).astype(jnp.bfloat16)

    def put_edge(side, even, odd):
        pedge_out[side, 0] = even.astype(jnp.bfloat16)
        pedge_out[side, 1] = odd.astype(jnp.bfloat16)

    def put_column(i, at):
        for k in range(4):
            xs[k + 1, at] = edge_in[i, k]
        xs[0, at] = roll_rows(edge_in[i, 3].astype(jnp.float32), 1).astype(jnp.bfloat16)
        xs[5, at] = roll_rows(edge_in[i, 0].astype(jnp.float32), -1).astype(jnp.bfloat16)

    def put_far(i):
        put_column(i, 2 - i + core * (cols + 1 + 2 * i))

    jp_near, jp_far = (1 - core) * (pcols - 1), core * (pcols - 1)
    jp_third = jp_far + wraps * (2 - jp_far)
    jp_fourth = 2 + jp_far - jp_third
    loads[1].wait()
    by_near.wait_recv()
    put_column(3, (1 - core) * (cols + 1) + 2)
    inside, beside_near = conv_first(1, jp_near)
    put_pooled(jp_near + 1, *beside_near)
    put_edge(0, *beside_near)
    put_pooled(2, *inside)
    by_near_2.start()

    hear(0)
    tell(1)

    @pl.when(first)
    def _():
        pl.semaphore_wait(barrier, 2)
        for copy in by_far:
            copy.start()

    @pl.when(inner)
    def _():
        by_far[0].wait_recv()
        put_far(0)

    (third,) = conv_first(jp_third)
    put_edge(1, *third)
    put_pooled(jp_third + 1, *third)

    @pl.when(inner)
    def _():
        by_far_2.start()

    hear(1)
    tell(2)

    @pl.when(wrap)
    def _():
        by_far[0].wait_recv()
        put_far(0)

    def conv_second(pieces):
        z = silu(jnp.dot(pieces, wb[...], preferred_element_type=jnp.float32))
        return z.reshape(2, 2, srows, z.shape[-1])

    loads[2].wait()
    loads[3].wait()
    (fourth,) = conv_first(jp_fourth)
    put_pooled(jp_fourth + 1, *fourth)
    chans = ps.shape[-1]
    inside = conv_second(
        jnp.concatenate(
            [
                ps[a : a + 2, 1 + b : 3 + b].reshape(4 * srows, chans)
                for a in range(3)
                for b in range(3)
            ],
            axis=1,
        )
    )
    hear(2)
    by_near_2.wait_recv()
    put_pooled(
        (1 - core) * (pcols + 1),
        pedge_in[0, 0].astype(jnp.float32),
        pedge_in[0, 1].astype(jnp.float32),
    )
    far_at = core * (pcols + 1)

    @pl.when(inner)
    def _():
        by_far_2.wait_recv()
        put_pooled(
            far_at, pedge_in[1, 0].astype(jnp.float32), pedge_in[1, 1].astype(jnp.float32)
        )

    @pl.when(wrap)
    def _():
        both = edge_in.at[pl.ds(1, 2)]
        halo(1, 0, both, both, beyond).wait_recv()
        put_far(1)
        put_far(2)
        put_pooled(far_at, *conv_first(core * (pcols + 1) - 1)[0])

    outer = conv_second(
        jnp.concatenate(
            [
                jnp.concatenate(
                    [
                        ps[a : a + 2, b].reshape(2 * srows, chans),
                        ps[a : a + 2, pcols - 1 + b].reshape(2 * srows, chans),
                    ],
                    axis=0,
                )
                for a in range(3)
                for b in range(3)
            ],
            axis=1,
        )
    )
    tokens = jnp.concatenate(
        [
            (inside[0, side] + inside[1, side] + outer[side, 0] + outer[side, 1]) * 0.25
            for side in range(2)
        ],
        axis=0,
    )
    centred = tokens - jnp.mean(tokens, axis=-1, keepdims=True)
    spread = jnp.mean(centred * centred, axis=-1, keepdims=True)
    normed = (centred * lax.rsqrt(spread + 0.01) * gain_ref[...]).astype(jnp.bfloat16)
    chunks = gat.shape[1]
    gat[me] = normed.reshape(gat.shape[1:])

    def send(block, ch, dev, sem):
        return pltpu.make_async_remote_copy(
            src_ref=gat.at[block, ch],
            dst_ref=gat.at[block, ch],
            send_sem=block_send,
            recv_sem=sem,
            device_id={"lon": dev},
        )

    def go(block, ch, dev):
        send(block, ch, dev, block_recv.at[block // 2, ch]).start()

    def beside(block, ch, unit):
        send(block, ch, other_core, side_recv.at[unit]).start()

    def arrived(block, ch):
        send(block, ch, other_core, block_recv.at[block // 2, ch]).wait_recv()

    for ch in range(chunks):
        go(me, ch, two * 4 + own)
        go(me, ch, other_x)
        beside(me, ch, 0)

    @pl.when(middle)
    def _():
        for ch in range(chunks):
            go(me, ch, rest * 4 + own)

    for ch in range(chunks):
        go(me, ch, near * 4 + mate)
    for ch in range(chunks):
        go(me, ch, near * 4 + own)

    loads[4].wait()
    group = 4 * hdim
    queries = jnp.dot(normed, wqkv[:, 0:width], preferred_element_type=jnp.float32)
    queries = queries.astype(jnp.bfloat16) * jnp.bfloat16(hdim**-0.5)
    lane_head = (lax.broadcasted_iota(jnp.int32, queries.shape, 1) % group) // hdim
    for a in range(4):
        qmask[a * toks : (a + 1) * toks, :] = jnp.where(
            lane_head == a, queries, jnp.zeros_like(queries)
        )
    heads_at = lax.broadcasted_iota(jnp.int32, (toks, group), 1) // hdim

    def by_head(v):
        got = v[0:toks]
        for a in range(1, 4):
            got = jnp.where(heads_at == a, v[a * toks : (a + 1) * toks], got)
        return got

    def project(unit, slot, chips):
        both = gat.at[pl.ds(0, len(chips))]
        pltpu.make_async_remote_copy(
            src_ref=both,
            dst_ref=both,
            send_sem=block_send,
            recv_sem=side_recv.at[unit],
            device_id={"lon": other_core},
        ).wait_recv()
        have = jnp.concatenate(
            [gat[pl.ds(2 * c, 2)].reshape(2 * toks, chans) for c in chips], axis=0
        )
        made = jnp.dot(have, wqkv[:, width:], preferred_element_type=jnp.float32)
        made = made.astype(jnp.bfloat16)
        at = slice(slot * 2 * toks, (slot + len(chips)) * 2 * toks)
        keys[at] = made[:, 0:width]
        vals[at] = made[:, width:]

    def attend(slots, end):
        at = slice(slots[0] * 2 * toks, slots[1] * 2 * toks)
        mixes, norms = {}, {}

        def score(g):
            lanes = slice(g * group, (g + 1) * group)
            scores = lax.dot_general(
                qmask[:, lanes],
                keys[at, lanes],
                (((1,), (1,)), ((), ())),
                preferred_element_type=jnp.float32,
            )
            peak = jnp.max(scores, axis=-1, keepdims=True)
            raised = jnp.exp(scores - peak)
            norms[g] = peak, jnp.sum(raised, axis=-1, keepdims=True)
            mixes[g] = raised.astype(jnp.bfloat16)

        def mix(g):
            lanes = slice(g * group, (g + 1) * group)
            mixed = jnp.dot(mixes[g], vals[at, lanes], preferred_element_type=jnp.float32)
            got, peak, total = by_head(mixed), by_head(norms[g][0]), by_head(norms[g][1])
            if end:
                top = jnp.maximum(peaks[:, lanes], peak)
                was, now = jnp.exp(peaks[:, lanes] - top), jnp.exp(peak - top)
                got = sums[:, lanes] * was + got * now
                total = totals[:, lanes] * was + total * now
                att[:, lanes] = (got * (1.0 / total)).astype(jnp.bfloat16)
            else:
                sums[:, lanes], totals[:, lanes], peaks[:, lanes] = got, total, peak

        groups = heads // 4
        for step in range(groups + 1):
            if step < groups:
                score(step)
            if step > 0:
                mix(step - 1)

    b_near, b_two, b_rest = near * 4 + own, two * 4 + own, rest * 4 + own
    c_near, c_two, c_rest = near * 4 + mate, two * 4 + mate, rest * 4 + mate

    def take(block, ch, unit, *onward):
        arrived(block, ch)
        for dev in onward:
            go(block, ch, dev)
        beside(block, ch, unit)

    def take_two(ch):
        arrived(b_two, ch)

        @pl.when(middle)
        def _():
            go(b_two, ch, rest * 4 + own)
            go(b_two, ch, rest * 4 + mate)

        go(b_two, ch, other_x)
        beside(b_two, ch, 1 + ends)

    def either(at_middle, at_end):
        return (at_middle + ends * (at_end - at_middle)) // 2

    project(0, 0, [me // 2])
    take(other_x, 0, 1)

    @pl.when(edge)
    def _():
        take(b_near, 0, 1, other_x)

    take(other_x, 1, 1)

    @pl.when(edge)
    def _():
        take(b_near, 1, 1, other_x)

    take_two(0)
    take_two(1)
    project(1, 1, [other_x // 2, either(b_two, b_near)])

    @pl.when(middle)
    def _():
        for ch in range(chunks):
            take(c_near, ch, 2)
            take(c_rest, ch, 3)
        for ch in range(chunks):
            take(b_rest, ch, 4)
            take(b_near, ch, 3)

    project(2, 3, [either(c_near, b_two)])
    attend((0, 4), False)

    @pl.when(edge)
    def _():
        take(c_near, 0, 3)
        take(c_near, 1, 3)
        take(b_rest, 0, 4)
        take(c_two, 0, 3)
        take(c_two, 1, 3)
        take(b_rest, 1, 4)
        take(c_rest, 0, 4)
        take(c_rest, 1, 4)

    @pl.when(middle)
    def _():
        take(c_two, 0, 4)
        take(c_two, 1, 4)

    project(3, 4, [either(c_rest, c_near), either(b_near, c_two)])
    project(4, 6, [b_rest // 2, either(c_two, c_rest)])
    attend((4, 8), True)

    loads[5].wait()
    final = tokens + jnp.dot(att[...], wo[...], preferred_element_type=jnp.float32)
    out_ref[...] = final.reshape(out_ref.shape).astype(jnp.bfloat16)

    def drain(ref, sem):
        pltpu.make_async_remote_copy(
            src_ref=ref,
            dst_ref=ref,
            send_sem=sem,
            recv_sem=halo_recv.at[0],
            device_id={"lon": other_core},
        ).wait_send()

    @pl.when(inner)
    def _():
        drain(edge_in.at[pl.ds(0, 2)], halo_send.at[0])
        drain(pedge_in, halo_send.at[1])

    @pl.when(wrap)
    def _():
        drain(edge_in, halo_send.at[0])
        drain(pedge_in.at[0], halo_send.at[1])

    @pl.when(middle)
    def _():
        drain(gat, block_send)

    @pl.when(edge)
    def _():
        drain(gat.at[pl.ds(0, n - 2)], block_send)


def fast_body(n, surface_field, conv_a, conv_b, norm_gain, qkv_weight, out_weight):
    rows, cols, chans_in = surface_field.shape
    chans = conv_a.shape[-1]
    srows, tcols = rows // 4, cols // 4
    toks = srows * tcols
    width = out_weight.shape[0]
    heads = width // HEAD_DIM
    bf16, f32 = jnp.bfloat16, jnp.float32
    vm, anyw = pl.BlockSpec(memory_space=pltpu.VMEM), pl.BlockSpec(memory_space=pltpu.HBM)
    out = pl.pallas_call(
        functools.partial(fused_kernel, n, cols, toks, heads, HEAD_DIM),
        out_shape=pltpu.VMEM((tcols, srows, chans), bf16),
        in_specs=[anyw] * 6,
        out_specs=vm,
        scratch_shapes=[
            pltpu.VMEM((rows * cols, chans_in), bf16),
            pltpu.VMEM((9 * chans_in, chans), bf16),
            pltpu.VMEM((9 * chans, chans), bf16),
            pltpu.VMEM(qkv_weight.shape, bf16),
            pltpu.VMEM(out_weight.shape, bf16),
            pltpu.VMEM((1, chans), f32),
            pltpu.VMEM((6, cols + 6, srows, chans_in), bf16),
            pltpu.VMEM((4, 4, srows, chans_in), bf16),
            pltpu.VMEM((4, cols // 2 + 2, srows, chans), bf16),
            pltpu.VMEM((2, 2, srows, chans), bf16),
            pltpu.VMEM((2, 2, srows, chans), bf16),
            pltpu.VMEM((n, CHUNKS, toks // CHUNKS, chans), bf16),
            pltpu.VMEM((n * toks, width), bf16),
            pltpu.VMEM((n * toks, width), bf16),
            pltpu.VMEM((toks, width), f32),
            pltpu.VMEM((toks, width), f32),
            pltpu.VMEM((toks, width), f32),
            pltpu.VMEM((4 * toks, width), bf16),
            pltpu.VMEM((toks, width), bf16),
            pltpu.SemaphoreType.DMA((6,)),
            pltpu.SemaphoreType.REGULAR,
            pltpu.SemaphoreType.REGULAR((3, 2)),
            pltpu.SemaphoreType.DMA((2,)),
            pltpu.SemaphoreType.DMA((5,)),
            pltpu.SemaphoreType.DMA,
            pltpu.SemaphoreType.DMA((n // 2, CHUNKS)),
            pltpu.SemaphoreType.DMA((5,)),
        ],
        compiler_params=pltpu.CompilerParams(
            collective_id=0, has_side_effects=True, vmem_limit_bytes=48 * 2**20
        ),
    )(
        *(
            pltpu.with_memory_space_constraint(v, pltpu.HBM)
            for v in (
                surface_field.reshape(rows * cols, chans_in),
                conv_a.reshape(9 * chans_in, chans),
                conv_b.reshape(9 * chans, chans),
                norm_gain.reshape(1, chans),
                qkv_weight,
                out_weight,
            )
        )
    )
    return out.transpose(1, 0, 2)


def solution(mesh):
    n = mesh.shape["lon"]
    plain = mesh.shape["lat"] > 1 or n != 16
    run = body if plain else functools.partial(fast_body, n)
    in_specs = (P(("grp", "lat"), "lon", None), P(), P(), P(), P(), P())
    out_specs = P(("grp", "lat"), "lon", None)
    return jax.shard_map(run, mesh=mesh, in_specs=in_specs, out_specs=out_specs, check_vma=False)
```

```python
import functools

import jax
import jax.numpy as jnp
from jax import lax
from jax.experimental import pallas as pl
from jax.experimental.pallas import tpu as pltpu
from jax.sharding import PartitionSpec as P

CB = 512
HEADS = 16
HEAD_DIM = 64
CHUNKS = 2


def with_halo(block, sides, width):
    for axis, dim in sides:
        count = lax.axis_size(axis)
        forward = [(i, i + 1) for i in range(count - 1)]
        forward.append((count - 1, 0))
        backward = [(target, source) for source, target in forward]
        low = lax.ppermute(
            lax.slice_in_dim(block, block.shape[dim] - width, None, axis=dim), axis, forward
        )
        high = lax.ppermute(lax.slice_in_dim(block, 0, width, axis=dim), axis, backward)
        block = jnp.concatenate([low, block, high], axis=dim)
    return block


def partner_2(value, axis, distance):
    mask = 2**distance
    pairs = [(source, source ^ mask) for source in range(lax.axis_size(axis))]
    return lax.ppermute(value, axis, pairs)


def convolve(values_in, weight):
    return lax.conv_general_dilated(
        values_in[None],
        weight,
        (1, 1),
        "VALID",
        dimension_numbers=("NHWC", "HWIO", "NHWC"),
        preferred_element_type=jnp.float32,
    )[0]


def average_pool(values_in):
    rows_in, cols_in, chans_in = values_in.shape
    return values_in.reshape(rows_in // 2, 2, cols_in // 2, 2, chans_in).mean(axis=(1, 3))


def layer_norm(tokens_flat, norm_gain):
    centred = tokens_flat - jnp.mean(tokens_flat, axis=-1, keepdims=True)
    spread = jnp.mean(centred * centred, axis=-1, keepdims=True)
    return centred * lax.rsqrt(spread + 0.01) * norm_gain


def softmax_rows(scores):
    maxima = jnp.max(scores, axis=-1, keepdims=True)
    raised = jnp.exp(scores - maxima)
    return raised / jnp.sum(raised, axis=-1, keepdims=True)


def keep_rows(values_in, rows_here, lat_count, lat_where, margin):
    first_row = lat_where * rows_here - margin
    rowpos = first_row + jnp.arange(values_in.shape[0], dtype=jnp.int32)
    inside = (rowpos >= 0) & (rowpos < rows_here * lat_count)
    return jnp.where(inside[:, None, None], values_in, jnp.zeros((), values_in.dtype))


def body(surface_field, conv_a, conv_b, norm_gain, qkv_weight, out_weight):
    lon_count = lax.axis_size("lon")
    lat_count = lax.axis_size("lat")
    lat_where = lax.axis_index("lat")
    rows_here = surface_field.shape[0]
    padded_field = with_halo(surface_field, (("lon", 1), ("lat", 0)), 1)
    padded_field = keep_rows(padded_field, rows_here, lat_count, lat_where, 1)
    first_out = jax.nn.silu(convolve(padded_field, conv_a))
    pooled_first = average_pool(first_out).astype(jnp.bfloat16)
    ready_rows = with_halo(pooled_first, (("lon", 1), ("lat", 0)), 1)
    ready_rows = keep_rows(ready_rows, rows_here // 2, lat_count, lat_where, 1)
    second_out = jax.nn.silu(convolve(ready_rows, conv_b))
    pooled_second = average_pool(second_out)
    tok_rows, tok_cols = (pooled_second.shape[0], pooled_second.shape[1])
    local_tokens = tok_rows * tok_cols
    tokens_flat = pooled_second.reshape(local_tokens, CB)
    normed = layer_norm(tokens_flat, norm_gain).astype(jnp.bfloat16)
    projected = jnp.dot(normed, qkv_weight, preferred_element_type=jnp.float32).astype(jnp.bfloat16)
    residues = max(1, lon_count // HEADS)
    groups = lon_count // residues
    per_slot = HEADS // groups
    per_residue = local_tokens // residues
    arranged = projected.reshape(per_residue, residues, 3, groups, per_slot, HEAD_DIM)
    outgoing = arranged.transpose(2, 1, 3, 4, 0, 5).reshape(
        3, lon_count, per_slot, per_residue, HEAD_DIM
    )
    swap_bits = list(range(groups.bit_length() - 1, lon_count.bit_length() - 1))
    arrived = lax.all_to_all(outgoing, "lon", split_axis=1, concat_axis=3, tiled=True)
    queries = arrived[0, 0]
    keys_vals = arrived[1:, 0]
    for bit_pos in swap_bits:
        partner = partner_2(keys_vals, "lon", bit_pos)
        keys_vals = jnp.concatenate([keys_vals, partner], axis=2)
    for bit_pos in range(lat_count.bit_length() - 1):
        partner = partner_2(keys_vals, "lat", bit_pos)
        keys_vals = jnp.concatenate([keys_vals, partner], axis=2)
    score_scale = HEAD_DIM ** (-0.5)
    scores = (
        jnp.einsum("hqd,hkd->hqk", queries, keys_vals[0], preferred_element_type=jnp.float32)
        * score_scale
    )
    weights = softmax_rows(scores).astype(jnp.bfloat16)
    head_out = jnp.einsum(
        "hqk,hkd->hqd", weights, keys_vals[1], preferred_element_type=jnp.float32
    ).astype(jnp.bfloat16)
    returned = lax.all_to_all(head_out[None], "lon", split_axis=2, concat_axis=0, tiled=True)
    attended = returned.reshape(residues, groups, per_slot, per_residue, HEAD_DIM).transpose(
        3, 0, 1, 2, 4
    )
    attended = attended.reshape(local_tokens, HEADS * HEAD_DIM)
    mixed_out = tokens_flat + jnp.dot(attended, out_weight, preferred_element_type=jnp.float32)
    return mixed_out.reshape(tok_rows, tok_cols, CB).astype(jnp.bfloat16)


def roll_rows(values, amount):
    count = values.shape[0]
    moved = pltpu.roll(values, amount % count, 0)
    rowpos = lax.broadcasted_iota(jnp.int32, values.shape, 0)
    edge = 0 if amount == 1 else count - 1
    return jnp.where(rowpos == edge, jnp.zeros_like(moved), moved)


def silu(v):
    half = 0.5 * v
    return half + half * jnp.tanh(half)


def fused_kernel(
    n, cols, toks, heads, hdim,
    x_hbm, wa_hbm, wb_hbm, gain_hbm, wqkv_hbm, wo_hbm, out_ref,
    x_v, wa, wb, wqkv, wo, gain_ref, xs, edge_in, ps, pedge_out, pedge_in,
    gat, keys, vals, sums, totals, peaks, qmask,
    load_sem, near_ok, told, halo_send, halo_recv, block_send, block_recv, side_recv,
):
    width = heads * hdim
    me = lax.axis_index("lon")
    core, x_at, z_at = me % 2, (me // 2) % 2, me // 4
    other_core = me + 1 - 2 * core
    other_x = me + 2 - 4 * x_at
    beyond = (me + n - 1 + 2 * core) % n
    wraps = me // (n - 1) + (n - 1 - me) // (n - 1)
    first, last = me == 0, me == n - 1
    wrap, inner = first | last, (me > 0) & (me < n - 1)
    near, two = z_at + 1 - 2 * (z_at // 2), (z_at + 2) % 4
    rest = (near + 2) % 4
    ends = z_at // 3 + (3 - z_at) // 3
    middle, edge = (z_at > 0) & (z_at < 3), (z_at == 0) | (z_at == 3)
    own, mate = me % 4, other_x % 4

    loads = [
        pltpu.make_async_copy(s, d, load_sem.at[i])
        for i, (s, d) in enumerate(
            (
                (x_hbm, x_v), (wa_hbm, wa), (wb_hbm, wb),
                (gain_hbm, gain_ref), (wqkv_hbm, wqkv), (wo_hbm, wo),
            )
        )
    ]
    for c in loads:
        c.start()

    barrier = pltpu.get_barrier_semaphore()

    def greet(dev):
        pl.semaphore_signal(barrier, inc=1, device_id={"lon": dev})

    greet(other_core)
    greet(beyond)

    srows = x_v.shape[0] // cols // 4
    span = 32 * cols
    row = lax.broadcasted_iota(jnp.int32, (span, span), 0)
    col = lax.broadcasted_iota(jnp.int32, (span, span), 1)
    source = (4 * (row % 8) + row // (8 * cols)) * cols + (row // 8) % cols
    order = jnp.where(col == source, 1.0, 0.0).astype(jnp.bfloat16)
    loads[0].wait()
    turned = [
        jnp.dot(order, x_v[at : at + span, :], preferred_element_type=jnp.float32)
        for at in range(0, x_v.shape[0], span)
    ]

    def column(k, j):
        at = (k * cols + j) * 8
        return jnp.concatenate([t[at : at + 8] for t in turned], axis=0)

    for j in range(cols):
        for k in range(4):
            xs[k + 1, j + 3] = column(k, j).astype(jnp.bfloat16)

    def halo(i, k, src, dst, dev):
        return pltpu.make_async_remote_copy(
            src_ref=src,
            dst_ref=dst,
            send_sem=halo_send.at[k],
            recv_sem=halo_recv.at[i],
            device_id={"lon": dev},
        )

    def edge_column(j):
        return xs.at[pl.ds(1, 4), j + 3]

    by_near = halo(3, 0, edge_column((1 - core) * (cols - 1)), edge_in.at[3], other_core)
    by_far = [
        halo(
            min(i, 1), 0, edge_column(core * (cols - 1) + (1 - 2 * core) * i), edge_in.at[i], beyond
        )
        for i in range(3)
    ]
    by_near_2 = halo(4, 1, pedge_out.at[0], pedge_in.at[0], other_core)
    by_far_2 = halo(2, 1, pedge_out.at[1], pedge_in.at[1], beyond)

    @pl.when(me > 0)
    def _():
        pl.semaphore_wait(barrier, 2)

    @pl.when(first)
    def _():
        pl.semaphore_wait(near_ok, 1)

    @pl.when(me == 1)
    def _():
        pl.semaphore_signal(near_ok, inc=1, device_id={"lon": other_core})

    @pl.when(me > 0)
    def _():
        by_far[0].start()

    by_near.start()

    @pl.when(last)
    def _():
        by_far[1].start()
        by_far[2].start()

    def tell(level):
        step = 2**level
        for way, dev, real in ((0, me + step, me < n - step), (1, me - step, me >= step)):

            @pl.when(real)
            def _(way=way, dev=dev):
                pl.semaphore_signal(told.at[level, way], inc=1, device_id={"lon": dev})

    def hear(level):
        step = 2**level
        for way, real in ((1, me < n - step), (0, me >= step)):

            @pl.when(real)
            def _(way=way):
                pl.semaphore_wait(told.at[level, way], 1)

    tell(0)
    for j in range(cols):
        xs[0, j + 3] = roll_rows(column(3, j), 1).astype(jnp.bfloat16)
        xs[5, j + 3] = roll_rows(column(0, j), -1).astype(jnp.bfloat16)

    pcols = cols // 2

    def conv_first(*jps):
        taps = [
            jnp.concatenate(
                [
                    xs[a : a + 4, pl.ds(2 * jp + 2 + b, 2)].reshape(8 * srows, xs.shape[-1])
                    for jp in jps
                ],
                axis=0,
            )
            for a in range(3)
            for b in range(3)
        ]
        y = silu(
            jnp.dot(jnp.concatenate(taps, axis=1), wa[...], preferred_element_type=jnp.float32)
        )
        y = y.reshape(len(jps), 4, 2, srows, y.shape[-1])
        return [
            [
                (y[i, k, 0] + y[i, k, 1] + y[i, k + 1, 0] + y[i, k + 1, 1]) * 0.25
                for k in (0, 2)
            ]
            for i in range(len(jps))
        ]

    def put_pooled(at, even, odd):
        ps[0, at] = roll_rows(odd, 1).astype(jnp.bfloat16)
        ps[1, at] = even.astype(jnp.bfloat16)
        ps[2, at] = odd.astype(jnp.bfloat16)
        ps[3, at] = roll_rows(even, -1).astype(jnp.bfloat16)

    def put_edge(side, even, odd):
        pedge_out[side, 0] = even.astype(jnp.bfloat16)
        pedge_out[side, 1] = odd.astype(jnp.bfloat16)

    def put_column(i, at):
        for k in range(4):
            xs[k + 1, at] = edge_in[i, k]
        xs[0, at] = roll_rows(edge_in[i, 3].astype(jnp.float32), 1).astype(jnp.bfloat16)
        xs[5, at] = roll_rows(edge_in[i, 0].astype(jnp.float32), -1).astype(jnp.bfloat16)

    def put_far(i):
        put_column(i, 2 - i + core * (cols + 1 + 2 * i))

    jp_near, jp_far = (1 - core) * (pcols - 1), core * (pcols - 1)
    jp_third = jp_far + wraps * (2 - jp_far)
    jp_fourth = 2 + jp_far - jp_third
    loads[1].wait()
    by_near.wait_recv()
    put_column(3, (1 - core) * (cols + 1) + 2)
    inside, beside_near = conv_first(1, jp_near)
    put_pooled(jp_near + 1, *beside_near)
    put_edge(0, *beside_near)
    put_pooled(2, *inside)
    by_near_2.start()

    hear(0)
    tell(1)

    @pl.when(first)
    def _():
        pl.semaphore_wait(barrier, 2)
        for copy in by_far:
            copy.start()

    @pl.when(inner)
    def _():
        by_far[0].wait_recv()
        put_far(0)

    (third,) = conv_first(jp_third)
    put_edge(1, *third)
    put_pooled(jp_third + 1, *third)

    @pl.when(inner)
    def _():
        by_far_2.start()

    hear(1)
    tell(2)

    @pl.when(wrap)
    def _():
        by_far[0].wait_recv()
        put_far(0)

    def conv_second(pieces):
        z = silu(jnp.dot(pieces, wb[...], preferred_element_type=jnp.float32))
        return z.reshape(2, 2, srows, z.shape[-1])

    loads[2].wait()
    loads[3].wait()
    (fourth,) = conv_first(jp_fourth)
    put_pooled(jp_fourth + 1, *fourth)
    chans = ps.shape[-1]
    inside = conv_second(
        jnp.concatenate(
            [
                ps[a : a + 2, 1 + b : 3 + b].reshape(4 * srows, chans)
                for a in range(3)
                for b in range(3)
            ],
            axis=1,
        )
    )
    hear(2)
    by_near_2.wait_recv()
    put_pooled(
        (1 - core) * (pcols + 1),
        pedge_in[0, 0].astype(jnp.float32),
        pedge_in[0, 1].astype(jnp.float32),
    )
    far_at = core * (pcols + 1)

    @pl.when(inner)
    def _():
        by_far_2.wait_recv()
        put_pooled(
            far_at, pedge_in[1, 0].astype(jnp.float32), pedge_in[1, 1].astype(jnp.float32)
        )

    @pl.when(wrap)
    def _():
        both = edge_in.at[pl.ds(1, 2)]
        halo(1, 0, both, both, beyond).wait_recv()
        put_far(1)
        put_far(2)
        put_pooled(far_at, *conv_first(core * (pcols + 1) - 1)[0])

    outer = conv_second(
        jnp.concatenate(
            [
                jnp.concatenate(
                    [
                        ps[a : a + 2, b].reshape(2 * srows, chans),
                        ps[a : a + 2, pcols - 1 + b].reshape(2 * srows, chans),
                    ],
                    axis=0,
                )
                for a in range(3)
                for b in range(3)
            ],
            axis=1,
        )
    )
    tokens = jnp.concatenate(
        [
            (inside[0, side] + inside[1, side] + outer[side, 0] + outer[side, 1]) * 0.25
            for side in range(2)
        ],
        axis=0,
    )
    centred = tokens - jnp.mean(tokens, axis=-1, keepdims=True)
    spread = jnp.mean(centred * centred, axis=-1, keepdims=True)
    normed = (centred * lax.rsqrt(spread + 0.01) * gain_ref[...]).astype(jnp.bfloat16)
    chunks = gat.shape[1]
    gat[me] = normed.reshape(gat.shape[1:])

    def send(block, ch, dev, sem):
        return pltpu.make_async_remote_copy(
            src_ref=gat.at[block, ch],
            dst_ref=gat.at[block, ch],
            send_sem=block_send,
            recv_sem=sem,
            device_id={"lon": dev},
        )

    def go(block, ch, dev):
        send(block, ch, dev, block_recv.at[block // 2, ch]).start()

    def beside(block, ch, unit):
        send(block, ch, other_core, side_recv.at[unit]).start()

    def arrived(block, ch):
        send(block, ch, other_core, block_recv.at[block // 2, ch]).wait_recv()

    for ch in range(chunks):
        go(me, ch, two * 4 + own)
        go(me, ch, other_x)
        beside(me, ch, 0)

    @pl.when(middle)
    def _():
        for ch in range(chunks):
            go(me, ch, rest * 4 + own)

    for ch in range(chunks):
        go(me, ch, near * 4 + mate)
    for ch in range(chunks):
        go(me, ch, near * 4 + own)

    loads[4].wait()
    group = 4 * hdim
    queries = jnp.dot(normed, wqkv[:, 0:width], preferred_element_type=jnp.float32)
    queries = queries.astype(jnp.bfloat16) * jnp.bfloat16(hdim**-0.5)
    lane_head = (lax.broadcasted_iota(jnp.int32, queries.shape, 1) % group) // hdim
    for a in range(4):
        qmask[a * toks : (a + 1) * toks, :] = jnp.where(
            lane_head == a, queries, jnp.zeros_like(queries)
        )
    heads_at = lax.broadcasted_iota(jnp.int32, (toks, group), 1) // hdim

    def by_head(v):
        got = v[0:toks]
        for a in range(1, 4):
            got = jnp.where(heads_at == a, v[a * toks : (a + 1) * toks], got)
        return got

    def side(unit, count):
        both = gat.at[pl.ds(0, count)]
        pltpu.make_async_remote_copy(
            src_ref=both,
            dst_ref=both,
            send_sem=block_send,
            recv_sem=side_recv.at[unit],
            device_id={"lon": other_core},
        ).wait_recv()

    def gathered(chips):
        return jnp.concatenate(
            [gat[pl.ds(2 * c, 2)].reshape(2 * toks, chans) for c in chips], axis=0
        )

    def project(unit, slot, chips):
        side(unit, len(chips))
        have = gathered(chips)
        made = jnp.dot(have, wqkv[:, width:], preferred_element_type=jnp.float32)
        made = made.astype(jnp.bfloat16)
        at = slice(slot * 2 * toks, (slot + len(chips)) * 2 * toks)
        keys[at] = made[:, 0:width]
        vals[at] = made[:, width:]

    def attend(made, done):
        held, ahead = {}, {}

        def score(g):
            lanes = slice(g * group, (g + 1) * group)
            these, those = ahead.pop(g)
            scores = lax.dot_general(
                qmask[:, lanes],
                these,
                (((1,), (1,)), ((), ())),
                preferred_element_type=jnp.float32,
            )
            peak = jnp.max(scores, axis=-1, keepdims=True)
            raised = jnp.exp(scores - peak)
            total = jnp.sum(raised, axis=-1, keepdims=True)
            held[g] = raised.astype(jnp.bfloat16), those, peak, total

        def mix(g):
            raised, those, peak, total = held.pop(g)
            mixed = jnp.dot(raised, those, preferred_element_type=jnp.float32)
            done(g, by_head(mixed), by_head(peak), by_head(total))

        groups = heads // 4
        ahead[0] = made(0)
        for step in range(groups + 1):
            if step + 1 < groups:
                ahead[step + 1] = made(step + 1)
            if step < groups:
                score(step)
            if step > 0:
                mix(step - 1)

    def stored(g):
        lanes = slice(g * group, (g + 1) * group)
        return keys[:, lanes], vals[:, lanes]

    def keep(g, got, peak, total):
        lanes = slice(g * group, (g + 1) * group)
        sums[:, lanes], totals[:, lanes], peaks[:, lanes] = got, total, peak

    def finish(g, got, peak, total):
        lanes = slice(g * group, (g + 1) * group)
        top = jnp.maximum(peaks[:, lanes], peak)
        was, now = jnp.exp(peaks[:, lanes] - top), jnp.exp(peak - top)
        got = sums[:, lanes] * was + got * now
        total = totals[:, lanes] * was + total * now
        att = (got * (1.0 / total)).astype(jnp.bfloat16)
        parts.append(jnp.dot(att, wo[lanes, :], preferred_element_type=jnp.float32))

    b_near, b_two, b_rest = near * 4 + own, two * 4 + own, rest * 4 + own
    c_near, c_two, c_rest = near * 4 + mate, two * 4 + mate, rest * 4 + mate

    def take(block, ch, unit, *onward):
        arrived(block, ch)
        for dev in onward:
            go(block, ch, dev)
        beside(block, ch, unit)

    def take_two(ch):
        arrived(b_two, ch)

        @pl.when(middle)
        def _():
            go(b_two, ch, rest * 4 + own)
            go(b_two, ch, rest * 4 + mate)

        go(b_two, ch, other_x)
        beside(b_two, ch, 1 + ends)

    def either(at_middle, at_end):
        return (at_middle + ends * (at_end - at_middle)) // 2

    project(0, 0, [me // 2])
    take(other_x, 0, 1)

    @pl.when(edge)
    def _():
        take(b_near, 0, 1, other_x)

    take(other_x, 1, 1)

    @pl.when(edge)
    def _():
        take(b_near, 1, 1, other_x)

    take_two(0)
    take_two(1)
    project(1, 1, [other_x // 2, either(b_two, b_near)])

    @pl.when(middle)
    def _():
        for ch in range(chunks):
            take(c_near, ch, 2)
            take(c_rest, ch, 3)
        for ch in range(chunks):
            take(b_rest, ch, 4)
            take(b_near, ch, 3)

    project(2, 3, [either(c_near, b_two)])
    attend(stored, keep)

    @pl.when(edge)
    def _():
        take(c_near, 0, 3)
        take(c_near, 1, 3)
        take(b_rest, 0, 4)
        take(c_two, 0, 3)
        take(c_two, 1, 3)
        take(b_rest, 1, 4)
        take(c_rest, 0, 4)
        take(c_rest, 1, 4)

    @pl.when(middle)
    def _():
        take(c_two, 0, 4)
        take(c_two, 1, 4)

    loads[5].wait()
    side(3, 2)
    side(4, 2)
    have = gathered(
        [
            either(c_rest, c_near), either(b_near, c_two),
            b_rest // 2, either(c_two, c_rest),
        ]
    )

    def fresh(g):
        return [
            jnp.dot(
                have,
                wqkv[:, at + g * group : at + (g + 1) * group],
                preferred_element_type=jnp.float32,
            ).astype(jnp.bfloat16)
            for at in (width, 2 * width)
        ]

    parts = []
    attend(fresh, finish)
    final = tokens + sum(parts)
    out_ref[...] = final.reshape(out_ref.shape).astype(jnp.bfloat16)

    def drain(ref, sem):
        pltpu.make_async_remote_copy(
            src_ref=ref,
            dst_ref=ref,
            send_sem=sem,
            recv_sem=halo_recv.at[0],
            device_id={"lon": other_core},
        ).wait_send()

    @pl.when(inner)
    def _():
        drain(edge_in.at[pl.ds(0, 2)], halo_send.at[0])
        drain(pedge_in, halo_send.at[1])

    @pl.when(wrap)
    def _():
        drain(edge_in, halo_send.at[0])
        drain(pedge_in.at[0], halo_send.at[1])

    @pl.when(middle)
    def _():
        drain(gat, block_send)

    @pl.when(edge)
    def _():
        drain(gat.at[pl.ds(0, n - 2)], block_send)


def fast_body(n, surface_field, conv_a, conv_b, norm_gain, qkv_weight, out_weight):
    rows, cols, chans_in = surface_field.shape
    chans = conv_a.shape[-1]
    srows, tcols = rows // 4, cols // 4
    toks = srows * tcols
    width = out_weight.shape[0]
    heads = width // HEAD_DIM
    bf16, f32 = jnp.bfloat16, jnp.float32
    vm, anyw = pl.BlockSpec(memory_space=pltpu.VMEM), pl.BlockSpec(memory_space=pltpu.HBM)
    out = pl.pallas_call(
        functools.partial(fused_kernel, n, cols, toks, heads, HEAD_DIM),
        out_shape=pltpu.VMEM((tcols, srows, chans), bf16),
        in_specs=[anyw] * 6,
        out_specs=vm,
        scratch_shapes=[
            pltpu.VMEM((rows * cols, chans_in), bf16),
            pltpu.VMEM((9 * chans_in, chans), bf16),
            pltpu.VMEM((9 * chans, chans), bf16),
            pltpu.VMEM(qkv_weight.shape, bf16),
            pltpu.VMEM(out_weight.shape, bf16),
            pltpu.VMEM((1, chans), f32),
            pltpu.VMEM((6, cols + 6, srows, chans_in), bf16),
            pltpu.VMEM((4, 4, srows, chans_in), bf16),
            pltpu.VMEM((4, cols // 2 + 2, srows, chans), bf16),
            pltpu.VMEM((2, 2, srows, chans), bf16),
            pltpu.VMEM((2, 2, srows, chans), bf16),
            pltpu.VMEM((n, CHUNKS, toks // CHUNKS, chans), bf16),
            pltpu.VMEM((n // 2 * toks, width), bf16),
            pltpu.VMEM((n // 2 * toks, width), bf16),
            pltpu.VMEM((toks, width), f32),
            pltpu.VMEM((toks, width), f32),
            pltpu.VMEM((toks, width), f32),
            pltpu.VMEM((4 * toks, width), bf16),
            pltpu.SemaphoreType.DMA((6,)),
            pltpu.SemaphoreType.REGULAR,
            pltpu.SemaphoreType.REGULAR((3, 2)),
            pltpu.SemaphoreType.DMA((2,)),
            pltpu.SemaphoreType.DMA((5,)),
            pltpu.SemaphoreType.DMA,
            pltpu.SemaphoreType.DMA((n // 2, CHUNKS)),
            pltpu.SemaphoreType.DMA((5,)),
        ],
        compiler_params=pltpu.CompilerParams(
            collective_id=0, has_side_effects=True, vmem_limit_bytes=48 * 2**20
        ),
    )(
        *(
            pltpu.with_memory_space_constraint(v, pltpu.HBM)
            for v in (
                surface_field.reshape(rows * cols, chans_in),
                conv_a.reshape(9 * chans_in, chans),
                conv_b.reshape(9 * chans, chans),
                norm_gain.reshape(1, chans),
                qkv_weight,
                out_weight,
            )
        )
    )
    return out.transpose(1, 0, 2)


def solution(mesh):
    n = mesh.shape["lon"]
    plain = mesh.shape["lat"] > 1 or n != 16
    run = body if plain else functools.partial(fast_body, n)
    in_specs = (P(("grp", "lat"), "lon", None), P(), P(), P(), P(), P())
    out_specs = P(("grp", "lat"), "lon", None)
    return jax.shard_map(run, mesh=mesh, in_specs=in_specs, out_specs=out_specs, check_vma=False)
```

```python
import functools

import jax
import jax.numpy as jnp
from jax import lax
from jax.experimental import pallas as pl
from jax.experimental.pallas import tpu as pltpu
from jax.sharding import PartitionSpec as P

CB = 512
HEADS = 16
HEAD_DIM = 64
CHUNKS = 2


def with_halo(block, sides, width):
    for axis, dim in sides:
        count = lax.axis_size(axis)
        forward = [(i, i + 1) for i in range(count - 1)]
        forward.append((count - 1, 0))
        backward = [(target, source) for source, target in forward]
        low = lax.ppermute(
            lax.slice_in_dim(block, block.shape[dim] - width, None, axis=dim), axis, forward
        )
        high = lax.ppermute(lax.slice_in_dim(block, 0, width, axis=dim), axis, backward)
        block = jnp.concatenate([low, block, high], axis=dim)
    return block


def partner_2(value, axis, distance):
    mask = 2**distance
    pairs = [(source, source ^ mask) for source in range(lax.axis_size(axis))]
    return lax.ppermute(value, axis, pairs)


def convolve(values_in, weight):
    return lax.conv_general_dilated(
        values_in[None],
        weight,
        (1, 1),
        "VALID",
        dimension_numbers=("NHWC", "HWIO", "NHWC"),
        preferred_element_type=jnp.float32,
    )[0]


def average_pool(values_in):
    rows_in, cols_in, chans_in = values_in.shape
    return values_in.reshape(rows_in // 2, 2, cols_in // 2, 2, chans_in).mean(axis=(1, 3))


def layer_norm(tokens_flat, norm_gain):
    centred = tokens_flat - jnp.mean(tokens_flat, axis=-1, keepdims=True)
    spread = jnp.mean(centred * centred, axis=-1, keepdims=True)
    return centred * lax.rsqrt(spread + 0.01) * norm_gain


def softmax_rows(scores):
    maxima = jnp.max(scores, axis=-1, keepdims=True)
    raised = jnp.exp(scores - maxima)
    return raised / jnp.sum(raised, axis=-1, keepdims=True)


def keep_rows(values_in, rows_here, lat_count, lat_where, margin):
    first_row = lat_where * rows_here - margin
    rowpos = first_row + jnp.arange(values_in.shape[0], dtype=jnp.int32)
    inside = (rowpos >= 0) & (rowpos < rows_here * lat_count)
    return jnp.where(inside[:, None, None], values_in, jnp.zeros((), values_in.dtype))


def body(surface_field, conv_a, conv_b, norm_gain, qkv_weight, out_weight):
    lon_count = lax.axis_size("lon")
    lat_count = lax.axis_size("lat")
    lat_where = lax.axis_index("lat")
    rows_here = surface_field.shape[0]
    padded_field = with_halo(surface_field, (("lon", 1), ("lat", 0)), 1)
    padded_field = keep_rows(padded_field, rows_here, lat_count, lat_where, 1)
    first_out = jax.nn.silu(convolve(padded_field, conv_a))
    pooled_first = average_pool(first_out).astype(jnp.bfloat16)
    ready_rows = with_halo(pooled_first, (("lon", 1), ("lat", 0)), 1)
    ready_rows = keep_rows(ready_rows, rows_here // 2, lat_count, lat_where, 1)
    second_out = jax.nn.silu(convolve(ready_rows, conv_b))
    pooled_second = average_pool(second_out)
    tok_rows, tok_cols = (pooled_second.shape[0], pooled_second.shape[1])
    local_tokens = tok_rows * tok_cols
    tokens_flat = pooled_second.reshape(local_tokens, CB)
    normed = layer_norm(tokens_flat, norm_gain).astype(jnp.bfloat16)
    projected = jnp.dot(normed, qkv_weight, preferred_element_type=jnp.float32).astype(jnp.bfloat16)
    residues = max(1, lon_count // HEADS)
    groups = lon_count // residues
    per_slot = HEADS // groups
    per_residue = local_tokens // residues
    arranged = projected.reshape(per_residue, residues, 3, groups, per_slot, HEAD_DIM)
    outgoing = arranged.transpose(2, 1, 3, 4, 0, 5).reshape(
        3, lon_count, per_slot, per_residue, HEAD_DIM
    )
    swap_bits = list(range(groups.bit_length() - 1, lon_count.bit_length() - 1))
    arrived = lax.all_to_all(outgoing, "lon", split_axis=1, concat_axis=3, tiled=True)
    queries = arrived[0, 0]
    keys_vals = arrived[1:, 0]
    for bit_pos in swap_bits:
        partner = partner_2(keys_vals, "lon", bit_pos)
        keys_vals = jnp.concatenate([keys_vals, partner], axis=2)
    for bit_pos in range(lat_count.bit_length() - 1):
        partner = partner_2(keys_vals, "lat", bit_pos)
        keys_vals = jnp.concatenate([keys_vals, partner], axis=2)
    score_scale = HEAD_DIM ** (-0.5)
    scores = (
        jnp.einsum("hqd,hkd->hqk", queries, keys_vals[0], preferred_element_type=jnp.float32)
        * score_scale
    )
    weights = softmax_rows(scores).astype(jnp.bfloat16)
    head_out = jnp.einsum(
        "hqk,hkd->hqd", weights, keys_vals[1], preferred_element_type=jnp.float32
    ).astype(jnp.bfloat16)
    returned = lax.all_to_all(head_out[None], "lon", split_axis=2, concat_axis=0, tiled=True)
    attended = returned.reshape(residues, groups, per_slot, per_residue, HEAD_DIM).transpose(
        3, 0, 1, 2, 4
    )
    attended = attended.reshape(local_tokens, HEADS * HEAD_DIM)
    mixed_out = tokens_flat + jnp.dot(attended, out_weight, preferred_element_type=jnp.float32)
    return mixed_out.reshape(tok_rows, tok_cols, CB).astype(jnp.bfloat16)


def roll_rows(values, amount):
    count = values.shape[0]
    moved = pltpu.roll(values, amount % count, 0)
    rowpos = lax.broadcasted_iota(jnp.int32, values.shape, 0)
    edge = 0 if amount == 1 else count - 1
    return jnp.where(rowpos == edge, jnp.zeros_like(moved), moved)


def silu(v):
    half = 0.5 * v
    return half + half * jnp.tanh(half)


def fused_kernel(
    n, cols, toks, heads, hdim,
    x_hbm, wa_hbm, wb_hbm, gain_hbm, wqkv_hbm, wo_hbm, out_ref,
    x_v, wa, wb, wqkv, wo, gain_ref, xs, edge_in, ps, pedge_out, pedge_in,
    gat, keys, vals, sums, totals, peaks, qmask,
    load_sem, near_ok, told, halo_send, halo_recv, block_send, block_recv, side_recv,
):
    width = heads * hdim
    me = lax.axis_index("lon")
    core, x_at, z_at = me % 2, (me // 2) % 2, me // 4
    other_core = me + 1 - 2 * core
    other_x = me + 2 - 4 * x_at
    beyond = (me + n - 1 + 2 * core) % n
    wraps = me // (n - 1) + (n - 1 - me) // (n - 1)
    first, last = me == 0, me == n - 1
    wrap, inner = first | last, (me > 0) & (me < n - 1)
    near, two = z_at + 1 - 2 * (z_at // 2), (z_at + 2) % 4
    rest = (near + 2) % 4
    ends = z_at // 3 + (3 - z_at) // 3
    middle, edge = (z_at > 0) & (z_at < 3), (z_at == 0) | (z_at == 3)
    own, mate = me % 4, other_x % 4

    loads = [
        pltpu.make_async_copy(s, d, load_sem.at[i])
        for i, (s, d) in enumerate(
            (
                (x_hbm, x_v), (wa_hbm, wa), (wb_hbm, wb),
                (gain_hbm, gain_ref), (wqkv_hbm, wqkv), (wo_hbm, wo),
            )
        )
    ]
    for c in loads:
        c.start()

    barrier = pltpu.get_barrier_semaphore()

    def greet(dev):
        pl.semaphore_signal(barrier, inc=1, device_id={"lon": dev})

    greet(other_core)
    greet(beyond)

    srows = x_v.shape[0] // cols // 4
    span = 32 * cols
    row = lax.broadcasted_iota(jnp.int32, (span, span), 0)
    col = lax.broadcasted_iota(jnp.int32, (span, span), 1)
    source = (4 * (row % 8) + row // (8 * cols)) * cols + (row // 8) % cols
    order = jnp.where(col == source, 1.0, 0.0).astype(jnp.bfloat16)
    loads[0].wait()
    turned = [
        jnp.dot(order, x_v[at : at + span, :], preferred_element_type=jnp.float32)
        for at in range(0, x_v.shape[0], span)
    ]

    def column(k, j):
        at = (k * cols + j) * 8
        return jnp.concatenate([t[at : at + 8] for t in turned], axis=0)

    for j in range(cols):
        for k in range(4):
            xs[k + 1, j + 3] = column(k, j).astype(jnp.bfloat16)

    def halo(i, k, src, dst, dev):
        return pltpu.make_async_remote_copy(
            src_ref=src,
            dst_ref=dst,
            send_sem=halo_send.at[k],
            recv_sem=halo_recv.at[i],
            device_id={"lon": dev},
        )

    def edge_column(j):
        return xs.at[pl.ds(1, 4), j + 3]

    by_near = halo(3, 0, edge_column((1 - core) * (cols - 1)), edge_in.at[3], other_core)
    by_far = [
        halo(
            min(i, 1), 0, edge_column(core * (cols - 1) + (1 - 2 * core) * i), edge_in.at[i], beyond
        )
        for i in range(3)
    ]
    by_near_2 = halo(4, 1, pedge_out.at[0], pedge_in.at[0], other_core)
    by_far_2 = halo(2, 1, pedge_out.at[1], pedge_in.at[1], beyond)

    @pl.when(me > 0)
    def _():
        pl.semaphore_wait(barrier, 2)

    @pl.when(first)
    def _():
        pl.semaphore_wait(near_ok, 1)

    @pl.when(me == 1)
    def _():
        pl.semaphore_signal(near_ok, inc=1, device_id={"lon": other_core})

    @pl.when(me > 0)
    def _():
        by_far[0].start()

    by_near.start()

    @pl.when(last)
    def _():
        by_far[1].start()
        by_far[2].start()

    def tell(level):
        step = 2**level
        for way, dev, real in ((0, me + step, me < n - step), (1, me - step, me >= step)):

            @pl.when(real)
            def _(way=way, dev=dev):
                pl.semaphore_signal(told.at[level, way], inc=1, device_id={"lon": dev})

    def hear(level):
        step = 2**level
        for way, real in ((1, me < n - step), (0, me >= step)):

            @pl.when(real)
            def _(way=way):
                pl.semaphore_wait(told.at[level, way], 1)

    tell(0)
    for j in range(cols):
        xs[0, j + 3] = roll_rows(column(3, j), 1).astype(jnp.bfloat16)
        xs[5, j + 3] = roll_rows(column(0, j), -1).astype(jnp.bfloat16)

    pcols = cols // 2

    def conv_first(*jps):
        taps = [
            jnp.concatenate(
                [
                    xs[a : a + 4, pl.ds(2 * jp + 2 + b, 2)].reshape(8 * srows, xs.shape[-1])
                    for jp in jps
                ],
                axis=0,
            )
            for a in range(3)
            for b in range(3)
        ]
        y = silu(
            jnp.dot(jnp.concatenate(taps, axis=1), wa[...], preferred_element_type=jnp.float32)
        )
        y = y.reshape(len(jps), 4, 2, srows, y.shape[-1])
        return [
            [
                (y[i, k, 0] + y[i, k, 1] + y[i, k + 1, 0] + y[i, k + 1, 1]) * 0.25
                for k in (0, 2)
            ]
            for i in range(len(jps))
        ]

    def put_pooled(at, even, odd):
        ps[0, at] = roll_rows(odd, 1).astype(jnp.bfloat16)
        ps[1, at] = even.astype(jnp.bfloat16)
        ps[2, at] = odd.astype(jnp.bfloat16)
        ps[3, at] = roll_rows(even, -1).astype(jnp.bfloat16)

    def put_edge(side, even, odd):
        pedge_out[side, 0] = even.astype(jnp.bfloat16)
        pedge_out[side, 1] = odd.astype(jnp.bfloat16)

    def put_column(i, at):
        for k in range(4):
            xs[k + 1, at] = edge_in[i, k]
        xs[0, at] = roll_rows(edge_in[i, 3].astype(jnp.float32), 1).astype(jnp.bfloat16)
        xs[5, at] = roll_rows(edge_in[i, 0].astype(jnp.float32), -1).astype(jnp.bfloat16)

    def put_far(i):
        put_column(i, 2 - i + core * (cols + 1 + 2 * i))

    jp_near, jp_far = (1 - core) * (pcols - 1), core * (pcols - 1)
    jp_third = jp_far + wraps * (2 - jp_far)
    jp_fourth = 2 + jp_far - jp_third
    loads[1].wait()
    (inside,) = conv_first(1)
    put_pooled(2, *inside)
    by_near.wait_recv()
    put_column(3, (1 - core) * (cols + 1) + 2)
    (beside_near,) = conv_first(jp_near)
    put_pooled(jp_near + 1, *beside_near)
    put_edge(0, *beside_near)
    by_near_2.start()

    hear(0)
    tell(1)

    @pl.when(first)
    def _():
        pl.semaphore_wait(barrier, 2)
        for copy in by_far:
            copy.start()

    @pl.when(inner)
    def _():
        by_far[0].wait_recv()
        put_far(0)

    (third,) = conv_first(jp_third)
    put_edge(1, *third)
    put_pooled(jp_third + 1, *third)

    @pl.when(inner)
    def _():
        by_far_2.start()

    hear(1)
    tell(2)

    @pl.when(wrap)
    def _():
        by_far[0].wait_recv()
        put_far(0)

    def conv_second(pieces):
        z = silu(jnp.dot(pieces, wb[...], preferred_element_type=jnp.float32))
        return z.reshape(2, 2, srows, z.shape[-1])

    loads[2].wait()
    loads[3].wait()
    (fourth,) = conv_first(jp_fourth)
    put_pooled(jp_fourth + 1, *fourth)
    chans = ps.shape[-1]
    inside = conv_second(
        jnp.concatenate(
            [
                ps[a : a + 2, 1 + b : 3 + b].reshape(4 * srows, chans)
                for a in range(3)
                for b in range(3)
            ],
            axis=1,
        )
    )
    hear(2)
    by_near_2.wait_recv()
    put_pooled(
        (1 - core) * (pcols + 1),
        pedge_in[0, 0].astype(jnp.float32),
        pedge_in[0, 1].astype(jnp.float32),
    )
    far_at = core * (pcols + 1)

    @pl.when(inner)
    def _():
        by_far_2.wait_recv()
        put_pooled(
            far_at, pedge_in[1, 0].astype(jnp.float32), pedge_in[1, 1].astype(jnp.float32)
        )

    @pl.when(wrap)
    def _():
        both = edge_in.at[pl.ds(1, 2)]
        halo(1, 0, both, both, beyond).wait_recv()
        put_far(1)
        put_far(2)
        put_pooled(far_at, *conv_first(core * (pcols + 1) - 1)[0])

    outer = conv_second(
        jnp.concatenate(
            [
                jnp.concatenate(
                    [
                        ps[a : a + 2, b].reshape(2 * srows, chans),
                        ps[a : a + 2, pcols - 1 + b].reshape(2 * srows, chans),
                    ],
                    axis=0,
                )
                for a in range(3)
                for b in range(3)
            ],
            axis=1,
        )
    )
    tokens = jnp.concatenate(
        [
            (inside[0, side] + inside[1, side] + outer[side, 0] + outer[side, 1]) * 0.25
            for side in range(2)
        ],
        axis=0,
    )
    centred = tokens - jnp.mean(tokens, axis=-1, keepdims=True)
    spread = jnp.mean(centred * centred, axis=-1, keepdims=True)
    normed = (centred * lax.rsqrt(spread + 0.01) * gain_ref[...]).astype(jnp.bfloat16)
    chunks = gat.shape[1]
    gat[me] = normed.reshape(gat.shape[1:])

    def send(block, ch, dev, sem):
        return pltpu.make_async_remote_copy(
            src_ref=gat.at[block, ch],
            dst_ref=gat.at[block, ch],
            send_sem=block_send,
            recv_sem=sem,
            device_id={"lon": dev},
        )

    def go(block, ch, dev):
        send(block, ch, dev, block_recv.at[block // 2, ch]).start()

    def beside(block, ch, unit):
        send(block, ch, other_core, side_recv.at[unit]).start()

    def arrived(block, ch):
        send(block, ch, other_core, block_recv.at[block // 2, ch]).wait_recv()

    for ch in range(chunks):
        go(me, ch, two * 4 + own)
        go(me, ch, other_x)
        beside(me, ch, 0)

    @pl.when(middle)
    def _():
        for ch in range(chunks):
            go(me, ch, rest * 4 + own)

    for ch in range(chunks):
        go(me, ch, near * 4 + mate)
    for ch in range(chunks):
        go(me, ch, near * 4 + own)

    loads[4].wait()
    group = 4 * hdim
    queries = jnp.dot(normed, wqkv[:, 0:width], preferred_element_type=jnp.float32)
    queries = queries.astype(jnp.bfloat16) * jnp.bfloat16(hdim**-0.5)
    lane_head = (lax.broadcasted_iota(jnp.int32, queries.shape, 1) % group) // hdim
    for a in range(4):
        qmask[a * toks : (a + 1) * toks, :] = jnp.where(
            lane_head == a, queries, jnp.zeros_like(queries)
        )
    heads_at = lax.broadcasted_iota(jnp.int32, (toks, group), 1) // hdim

    def by_head(v):
        got = v[0:toks]
        for a in range(1, 4):
            got = jnp.where(heads_at == a, v[a * toks : (a + 1) * toks], got)
        return got

    def side(unit, count):
        both = gat.at[pl.ds(0, count)]
        pltpu.make_async_remote_copy(
            src_ref=both,
            dst_ref=both,
            send_sem=block_send,
            recv_sem=side_recv.at[unit],
            device_id={"lon": other_core},
        ).wait_recv()

    def gathered(chips):
        return jnp.concatenate(
            [gat[pl.ds(2 * c, 2)].reshape(2 * toks, chans) for c in chips], axis=0
        )

    def project(unit, slot, chips):
        side(unit, len(chips))
        have = gathered(chips)
        made = jnp.dot(have, wqkv[:, width:], preferred_element_type=jnp.float32)
        made = made.astype(jnp.bfloat16)
        at = slice(slot * 2 * toks, (slot + len(chips)) * 2 * toks)
        keys[at] = made[:, 0:width]
        vals[at] = made[:, width:]

    def attend(made, done):
        held, ahead = {}, {}

        def score(g):
            lanes = slice(g * group, (g + 1) * group)
            these, those = ahead.pop(g)
            scores = lax.dot_general(
                qmask[:, lanes],
                these,
                (((1,), (1,)), ((), ())),
                preferred_element_type=jnp.float32,
            )
            peak = jnp.max(scores, axis=-1, keepdims=True)
            raised = jnp.exp(scores - peak)
            total = jnp.sum(raised, axis=-1, keepdims=True)
            held[g] = raised.astype(jnp.bfloat16), those, peak, total

        def mix(g):
            raised, those, peak, total = held.pop(g)
            mixed = jnp.dot(raised, those, preferred_element_type=jnp.float32)
            done(g, by_head(mixed), by_head(peak), by_head(total))

        groups = heads // 4
        ahead[0] = made(0)
        for step in range(groups + 1):
            if step + 1 < groups:
                ahead[step + 1] = made(step + 1)
            if step < groups:
                score(step)
            if step > 0:
                mix(step - 1)

    def stored(g):
        lanes = slice(g * group, (g + 1) * group)
        return keys[:, lanes], vals[:, lanes]

    def keep(g, got, peak, total):
        lanes = slice(g * group, (g + 1) * group)
        sums[:, lanes], totals[:, lanes], peaks[:, lanes] = got, total, peak

    def finish(g, got, peak, total):
        lanes = slice(g * group, (g + 1) * group)
        top = jnp.maximum(peaks[:, lanes], peak)
        was, now = jnp.exp(peaks[:, lanes] - top), jnp.exp(peak - top)
        got = sums[:, lanes] * was + got * now
        total = totals[:, lanes] * was + total * now
        att = (got * (1.0 / total)).astype(jnp.bfloat16)
        parts.append(jnp.dot(att, wo[lanes, :], preferred_element_type=jnp.float32))

    b_near, b_two, b_rest = near * 4 + own, two * 4 + own, rest * 4 + own
    c_near, c_two, c_rest = near * 4 + mate, two * 4 + mate, rest * 4 + mate

    def take(block, ch, unit, *onward):
        arrived(block, ch)
        for dev in onward:
            go(block, ch, dev)
        beside(block, ch, unit)

    def take_two(ch):
        arrived(b_two, ch)

        @pl.when(middle)
        def _():
            go(b_two, ch, rest * 4 + own)
            go(b_two, ch, rest * 4 + mate)

        go(b_two, ch, other_x)
        beside(b_two, ch, 1 + ends)

    def either(at_middle, at_end):
        return (at_middle + ends * (at_end - at_middle)) // 2

    project(0, 0, [me // 2])
    take(other_x, 0, 1)

    @pl.when(edge)
    def _():
        take(b_near, 0, 1, other_x)

    take(other_x, 1, 1)

    @pl.when(edge)
    def _():
        take(b_near, 1, 1, other_x)

    take_two(0)
    take_two(1)
    project(1, 1, [other_x // 2, either(b_two, b_near)])

    @pl.when(middle)
    def _():
        for ch in range(chunks):
            take(c_near, ch, 2)
            take(c_rest, ch, 3)
        for ch in range(chunks):
            take(b_rest, ch, 4)
            take(b_near, ch, 3)

    project(2, 3, [either(c_near, b_two)])
    attend(stored, keep)

    @pl.when(edge)
    def _():
        take(c_near, 0, 3)
        take(c_near, 1, 3)
        take(b_rest, 0, 4)
        take(c_two, 0, 3)
        take(c_two, 1, 3)
        take(b_rest, 1, 4)
        take(c_rest, 0, 4)
        take(c_rest, 1, 4)

    @pl.when(middle)
    def _():
        take(c_two, 0, 4)
        take(c_two, 1, 4)

    loads[5].wait()
    side(3, 2)
    side(4, 2)
    have = gathered(
        [
            either(c_rest, c_near), either(b_near, c_two),
            b_rest // 2, either(c_two, c_rest),
        ]
    )

    def fresh(g):
        return [
            jnp.dot(
                have,
                wqkv[:, at + g * group : at + (g + 1) * group],
                preferred_element_type=jnp.float32,
            ).astype(jnp.bfloat16)
            for at in (width, 2 * width)
        ]

    parts = []
    attend(fresh, finish)
    final = tokens + sum(parts)
    out_ref[...] = final.reshape(out_ref.shape).astype(jnp.bfloat16)

    def drain(ref, sem):
        pltpu.make_async_remote_copy(
            src_ref=ref,
            dst_ref=ref,
            send_sem=sem,
            recv_sem=halo_recv.at[0],
            device_id={"lon": other_core},
        ).wait_send()

    @pl.when(inner)
    def _():
        drain(edge_in.at[pl.ds(0, 2)], halo_send.at[0])
        drain(pedge_in, halo_send.at[1])

    @pl.when(wrap)
    def _():
        drain(edge_in, halo_send.at[0])
        drain(pedge_in.at[0], halo_send.at[1])

    @pl.when(middle)
    def _():
        drain(gat, block_send)

    @pl.when(edge)
    def _():
        drain(gat.at[pl.ds(0, n - 2)], block_send)


def fast_body(n, surface_field, conv_a, conv_b, norm_gain, qkv_weight, out_weight):
    rows, cols, chans_in = surface_field.shape
    chans = conv_a.shape[-1]
    srows, tcols = rows // 4, cols // 4
    toks = srows * tcols
    width = out_weight.shape[0]
    heads = width // HEAD_DIM
    bf16, f32 = jnp.bfloat16, jnp.float32
    vm, anyw = pl.BlockSpec(memory_space=pltpu.VMEM), pl.BlockSpec(memory_space=pltpu.HBM)
    out = pl.pallas_call(
        functools.partial(fused_kernel, n, cols, toks, heads, HEAD_DIM),
        out_shape=pltpu.VMEM((tcols, srows, chans), bf16),
        in_specs=[anyw] * 6,
        out_specs=vm,
        scratch_shapes=[
            pltpu.VMEM((rows * cols, chans_in), bf16),
            pltpu.VMEM((9 * chans_in, chans), bf16),
            pltpu.VMEM((9 * chans, chans), bf16),
            pltpu.VMEM(qkv_weight.shape, bf16),
            pltpu.VMEM(out_weight.shape, bf16),
            pltpu.VMEM((1, chans), f32),
            pltpu.VMEM((6, cols + 6, srows, chans_in), bf16),
            pltpu.VMEM((4, 4, srows, chans_in), bf16),
            pltpu.VMEM((4, cols // 2 + 2, srows, chans), bf16),
            pltpu.VMEM((2, 2, srows, chans), bf16),
            pltpu.VMEM((2, 2, srows, chans), bf16),
            pltpu.VMEM((n, CHUNKS, toks // CHUNKS, chans), bf16),
            pltpu.VMEM((n // 2 * toks, width), bf16),
            pltpu.VMEM((n // 2 * toks, width), bf16),
            pltpu.VMEM((toks, width), f32),
            pltpu.VMEM((toks, width), f32),
            pltpu.VMEM((toks, width), f32),
            pltpu.VMEM((4 * toks, width), bf16),
            pltpu.SemaphoreType.DMA((6,)),
            pltpu.SemaphoreType.REGULAR,
            pltpu.SemaphoreType.REGULAR((3, 2)),
            pltpu.SemaphoreType.DMA((2,)),
            pltpu.SemaphoreType.DMA((5,)),
            pltpu.SemaphoreType.DMA,
            pltpu.SemaphoreType.DMA((n // 2, CHUNKS)),
            pltpu.SemaphoreType.DMA((5,)),
        ],
        compiler_params=pltpu.CompilerParams(
            collective_id=0, has_side_effects=True, vmem_limit_bytes=48 * 2**20
        ),
    )(
        *(
            pltpu.with_memory_space_constraint(v, pltpu.HBM)
            for v in (
                surface_field.reshape(rows * cols, chans_in),
                conv_a.reshape(9 * chans_in, chans),
                conv_b.reshape(9 * chans, chans),
                norm_gain.reshape(1, chans),
                qkv_weight,
                out_weight,
            )
        )
    )
    return out.transpose(1, 0, 2)


def solution(mesh):
    n = mesh.shape["lon"]
    plain = mesh.shape["lat"] > 1 or n != 16
    run = body if plain else functools.partial(fast_body, n)
    in_specs = (P(("grp", "lat"), "lon", None), P(), P(), P(), P(), P())
    out_specs = P(("grp", "lat"), "lon", None)
    return jax.shard_map(run, mesh=mesh, in_specs=in_specs, out_specs=out_specs, check_vma=False)
```
